32 devices in a mesh: px: 8 (over z, y), py: 4 (over x, core).
Axes of the slice: x: 2, y: 2, z: 4, core: 2. Of those that a mesh axis runs over, the one named last changes fastest.
Arguments:
- flow_field: bfloat16 [64, 128, 128, 128], P(None, 'px', 'py'), may hold values from -6 to 6
- cotangent: bfloat16 [64, 128, 128, 128], P(None, 'px', 'py'), may hold values from -6 to 6
- tucker_core: float32 [16, 16, 8, 8, 8], replicated, may hold values from -6 to 6
- in_factor: float32 [64, 16], replicated, may hold values from -0.75 to 0.75
- out_factor: float32 [64, 16], replicated, may hold values from -1.5 to 1.5
- first_factor: float32 [32, 8], replicated, may hold values from -2 to 2
- second_factor: float32 [32, 8], replicated, may hold values from -2 to 2
- third_factor: float32 [32, 8], replicated, may hold values from -2 to 2
Outputs:
- output_field: bfloat16 [64, 128, 128, 128], P(None, 'px', 'py')
- core_grad: float32 [16, 16, 8, 8, 8], replicated
- in_grad: float32 [64, 16], replicated
- out_grad: float32 [64, 16], replicated
- first_grad: float32 [32, 8], replicated
- second_grad: float32 [32, 8], replicated
- third_grad: float32 [32, 8], replicated
The draws below stay inside these ranges and needn't reach their ends.
All inputs are finite; a program needn't handle non-finite values.
Results may differ from the reference program's by a relative error of at most 0.001.
Values sent between devices are 32-bit elements; how exact they have to be, the bound alone decides.
A program may use at most 192 MiB of HBM per device.

```python
import jax
import jax.numpy as jnp
from jax import lax

C = 64
NX = 128
NY = 128
NZ = 128
M1 = 32
M2 = 32
M3 = 32
RI = 16
RO = 16
R1 = 8
R2 = 8
R3 = 8


def block_scale(rng, extent, cuts, low, high):
    def one(position, shards_of):
        heights = jax.random.uniform(jax.random.fold_in(jax.random.fold_in(rng, 6), position), (shards_of,), jnp.float32, low / len(cuts), high / len(cuts))
        return jnp.repeat(jnp.exp(heights), extent[position] // shards_of).reshape((-1,) + (1,) * (len(extent) - position - 1))

    level = one(*cuts[0])
    for cut in cuts[1:]:
        level = level * one(*cut)
    return level


def centred(rng, shape, width, bound, pieces=(), kind=jnp.bfloat16):
    result = jax.random.normal(rng, shape, jnp.float32) * width
    if len(pieces) > 0:
        result = block_scale(rng, shape, pieces, -0.22, 0.18) * result
    return jnp.clip(result, min=-bound, max=bound).astype(kind)


def setup_inputs(seed: int = 0) -> dict:
    key_list = jax.random.split(jax.random.key(seed), 9)
    flow_field = centred(key_list[0], (C, NX, NY, NZ), 1.0, 6.0, ((1, 8), (2, 4)))
    cotangent = centred(key_list[1], (C, NX, NY, NZ), 1.0, 6.0, ((1, 8), (2, 4)))
    tucker_core = centred(key_list[2], (RI, RO, R1, R2, R3), (0.3 * ((NX * NY * NZ) // (2 * M1 * M2 * M3)) ** 0.5), 6.0, (), jnp.float32)
    in_factor = centred(key_list[3], (C, RI), C ** -0.5, 0.75, (), jnp.float32)
    out_factor = centred(key_list[4], (C, RO), RO ** -0.5, 1.5, (), jnp.float32)
    first_factor = centred(key_list[5], (M1, R1), R1 ** -0.5, 2.0, (), jnp.float32)
    second_factor = centred(key_list[6], (M2, R2), R2 ** -0.5, 2.0, (), jnp.float32)
    third_factor = centred(key_list[7], (M3, R3), R3 ** -0.5, 2.0, (), jnp.float32)
    return dict(flow_field=flow_field, cotangent=cotangent, tucker_core=tucker_core, in_factor=in_factor, out_factor=out_factor, first_factor=first_factor, second_factor=second_factor, third_factor=third_factor)


HIGHEST = lax.Precision.HIGHEST

def kept_index(count, length):
    half_count = count // 2
    return jnp.concatenate([jnp.arange(half_count), jnp.arange(length - half_count, length)]).astype(jnp.int32)

def spectrum(plane):
    whole = jnp.fft.rfftn(plane, axes=(0, 1, 2))
    rows_kept = kept_index(M1, NX)
    cols_kept = kept_index(M2, NY)
    trimmed = whole[rows_kept][:, cols_kept][:, :, :M3]
    return jnp.stack([jnp.real(trimmed), jnp.imag(trimmed)])

def to_grid(modes):
    values = modes[0] + 1j * modes[1]
    whole = jnp.zeros((NX, NY, NZ // 2 + 1), values.dtype)
    rows_kept = kept_index(M1, NX)
    cols_kept = kept_index(M2, NY)
    depth_kept = jnp.arange(M3).astype(jnp.int32)
    whole = whole.at[rows_kept[:, None, None], cols_kept[None, :, None], depth_kept[None, None, :]].set(values)
    return jnp.fft.irfftn(whole, s=(NX, NY, NZ), axes=(0, 1, 2))

def mixing(tucker_core, in_factor, out_factor, first_factor, second_factor, third_factor, spectra):
    partial_core = jnp.einsum('abrst,mt->abrsm', tucker_core, third_factor, precision=HIGHEST)
    partial_core = jnp.einsum('abrsm,ks->abrkm', partial_core, second_factor, precision=HIGHEST)
    kernel = jnp.einsum('abrkm,jr->abjkm', partial_core, first_factor, precision=HIGHEST)
    lifted = jnp.einsum('ia,ipjkm->apjkm', in_factor, spectra, precision=HIGHEST)
    mixed = jnp.einsum('abjkm,apjkm->bpjkm', kernel, lifted, precision=HIGHEST)
    return jnp.einsum('ob,bpjkm->opjkm', out_factor, mixed, precision=HIGHEST)

def reference(flow_field, cotangent, tucker_core, in_factor, out_factor, first_factor, second_factor, third_factor):
    spectra = lax.map(lambda plane: spectrum(plane.astype(jnp.float32)), flow_field)
    weights = jnp.where(jnp.arange(M3) == 0, 1.0, 2.0).astype(jnp.float32)
    inverse_count = 1.0 / (NX * NY * NZ)
    back = lax.map(lambda plane: spectrum(plane.astype(jnp.float32)), cotangent) * (weights * inverse_count)

    def forward(core_arg, in_arg, out_arg, first_arg, second_arg, third_arg):
        return mixing(core_arg, in_arg, out_arg, first_arg, second_arg, third_arg, spectra)
    joined, pullback = jax.vjp(forward, tucker_core, in_factor, out_factor, first_factor, second_factor, third_factor)
    grads = pullback(back)
    output_field = lax.map(lambda modes: to_grid(modes).astype(jnp.bfloat16), joined)
    return (output_field, grads[0], grads[1], grads[2], grads[3], grads[4], grads[5])
```

```python
import functools
import math

import jax
import jax.numpy as jnp
import numpy as np
from jax import lax
from jax.experimental import pallas as pl
from jax.experimental.pallas import tpu as pltpu
from jax.sharding import PartitionSpec as P

NX = 128
NY = 128
NZ = 128
M1 = 32
M2 = 32
M3 = 32


HIGHEST = lax.Precision.HIGHEST


def turn_table(count, length):
    position = jnp.arange(count)
    frequency = jnp.where(position < count // 2, position, position - count)
    cells_at = jnp.arange(length)
    phase = frequency[None, :] * cells_at[:, None] % length
    angle = 2.0 * math.pi / length * phase.astype(jnp.float32)
    cosine = jnp.cos(angle)
    sine = jnp.sin(angle)
    upper = jnp.stack([cosine, -sine], axis=1)
    lower = jnp.stack([sine, cosine], axis=1)
    return jnp.stack([upper, lower])


def depth_table(length, count):
    cells_at = jnp.arange(length)
    frequency = jnp.arange(count)
    phase = cells_at[:, None] * frequency[None, :] % length
    angle = 2.0 * math.pi / length * phase.astype(jnp.float32)
    return jnp.concatenate([jnp.cos(angle), -jnp.sin(angle)], axis=1)


def to_modes(fields, depth_tables):
    across = turn_table(M2, NY)
    along = turn_table(M1, NX)
    spectra = []
    for member, z_table in zip(fields, depth_tables):
        channels, rows_here, cols_here, depth_len = member.shape
        flat = jnp.dot(member.reshape(-1, depth_len), z_table, precision=HIGHEST)
        spectra.append(flat.reshape(channels, rows_here, cols_here, 2, M3))
    members = lax.all_to_all(tuple(spectra), "py", split_axis=4, concat_axis=2, tiled=True)
    lines = tuple(
        (jnp.einsum("cxypm,pyqk->cxqkm", member, across, precision=HIGHEST) for member in members)
    )
    members = (
        lax.all_to_all(lines[0], "px", split_axis=3, concat_axis=1, tiled=True),
        lax.all_to_all(lines[1], "px", split_axis=3, concat_axis=1, tiled=True),
    )
    return tuple(
        (jnp.einsum("cxpkm,pxqj->cqjkm", member, along, precision=HIGHEST) for member in members)
    )


def to_space(modes, depth_weights):
    across = turn_table(M2, NY)
    along = turn_table(M1, NX)
    depth_base = depth_table(NZ, M3).T.reshape(2, M3, NZ)
    lines = tuple(
        (jnp.einsum("cqjkm,pxqj->cpxkm", member, along, precision=HIGHEST) for member in modes)
    )
    members = (
        lax.all_to_all(lines[0], "px", split_axis=2, concat_axis=3, tiled=True),
        lax.all_to_all(lines[1], "px", split_axis=2, concat_axis=3, tiled=True),
    )
    columns = tuple(
        (jnp.einsum("cqxkm,pyqk->cpxym", member, across, precision=HIGHEST) for member in members)
    )
    members = (
        lax.all_to_all(columns[0], "py", split_axis=3, concat_axis=4, tiled=True),
        lax.all_to_all(columns[1], "py", split_axis=3, concat_axis=4, tiled=True),
    )
    return tuple(
        (
            jnp.einsum(
                "cpxyk,pkn->cxyn", member, depth_base * weight_row[None, :, None], precision=HIGHEST
            )
            for member, weight_row in zip(members, depth_weights)
        )
    )


def shards(
    flow_field,
    cotangent,
    tucker_core,
    in_factor,
    out_factor,
    first_factor,
    second_factor,
    third_factor,
):
    inverse_count = 1.0 / (NX * NY * NZ)
    weights = jnp.where(jnp.arange(M3) == 0, 1.0, 2.0).astype(jnp.float32)
    unit_weights = jnp.ones((M3,), jnp.float32)
    base_table = depth_table(NZ, M3)
    weighted_table = base_table * jnp.concatenate([weights, weights])[None, :]
    block_second = M2 // lax.axis_size("px")
    block_third = M3 // lax.axis_size("py")
    start_second = lax.axis_index("px") * block_second
    start_third = lax.axis_index("py") * block_third

    def build_kernel(core_arg, first_arg, second_arg, third_arg):
        second_rows = lax.dynamic_slice_in_dim(second_arg, start_second, block_second, 0)
        third_rows = lax.dynamic_slice_in_dim(third_arg, start_third, block_third, 0)
        partial_core = jnp.einsum("abrst,mt->abrsm", core_arg, third_rows, precision=HIGHEST)
        partial_core = jnp.einsum("abrsm,ks->abrkm", partial_core, second_rows, precision=HIGHEST)
        return jnp.einsum("abrkm,jr->abjkm", partial_core, first_arg, precision=HIGHEST)

    kernel, pullback = jax.vjp(build_kernel, tucker_core, first_factor, second_factor, third_factor)
    field_wide = flow_field.astype(jnp.float32)
    back_wide = cotangent.astype(jnp.float32)
    lifted_grid = jnp.einsum("cxyn,ca->axyn", field_wide, in_factor, precision=HIGHEST)
    back_grid = jnp.einsum("cxyn,cb->bxyn", back_wide, out_factor, precision=HIGHEST)
    lifted, back_mixed = to_modes((lifted_grid, back_grid), (base_table, weighted_table))
    back_mixed = back_mixed * inverse_count
    mixed = jnp.einsum("abjkm,apjkm->bpjkm", kernel, lifted, precision=HIGHEST)
    grad_kernel = jnp.einsum("bpjkm,apjkm->abjkm", back_mixed, lifted, precision=HIGHEST)
    back_lifted = jnp.einsum("abjkm,bpjkm->apjkm", kernel, back_mixed, precision=HIGHEST)
    mixed_grid, lifted_back = to_space((mixed, back_lifted), (weights, unit_weights))
    mixed_grid = mixed_grid * inverse_count
    output_field = jnp.einsum("ob,bxyn->oxyn", out_factor, mixed_grid, precision=HIGHEST).astype(
        jnp.bfloat16
    )
    grad_out = jnp.einsum("oxyn,bxyn->ob", back_wide, mixed_grid, precision=HIGHEST)
    grad_in = jnp.einsum("ixyn,axyn->ia", field_wide, lifted_back, precision=HIGHEST)
    grad_core, grad_first, grad_second, grad_third = pullback(grad_kernel)
    totals = lax.psum(
        (grad_core, grad_in, grad_out, grad_first, grad_second, grad_third), ("px", "py")
    )
    return (output_field, totals[0], totals[1], totals[2], totals[3], totals[4], totals[5])


BF16 = jnp.bfloat16
F32 = jnp.float32
NN = (((1,), (0,)), ((), ()))
NT = (((1,), (1,)), ((), ()))
TN = (((0,), (0,)), ((), ()))
MESH = pl.DeviceIdType.MESH
VMEM_LIMIT = 60 * 1024 * 1024
SUB = 16
LANES = 128


def mul(a, b, dims=NN):
    return lax.dot_general(a, b, dims, preferred_element_type=F32)


def exact(a, b, dims=NN):
    return lax.dot_general(a, b, dims, precision=HIGHEST, preferred_element_type=F32)


def halves(x):
    high = x.astype(BF16)
    return high, (x - high.astype(F32)).astype(BF16)


def mul3(a, b, dims=NN):
    (ah, al), (bh, bl) = a, b
    return mul(ah, bh, dims) + (mul(ah, bl, dims) + mul(al, bh, dims))


def np_halves(x):
    x = np.asarray(x, np.float32)
    high = x.astype(BF16)
    return np.stack([high, (x - high.astype(np.float32)).astype(BF16)])


def np_turn(count, length):
    position = np.arange(count)
    frequency = np.where(position < count // 2, position, position - count)
    phase = frequency[None, :] * np.arange(length)[:, None] % length
    angle = 2.0 * np.pi / length * phase
    upper = np.stack([np.cos(angle), -np.sin(angle)], axis=1)
    lower = np.stack([np.sin(angle), np.cos(angle)], axis=1)
    return np.stack([upper, lower])


def np_depth(length, count):
    phase = np.arange(length)[:, None] * np.arange(count)[None, :] % length
    angle = 2.0 * np.pi / length * phase
    return np.stack([np.cos(angle), -np.sin(angle)])


def iota(shape, axis):
    return lax.broadcasted_iota(jnp.int32, shape, axis)


def one_hot(rows, cols, row_of, col_of):
    return row_of(iota((rows, cols), 0)) == col_of(iota((rows, cols), 1))


def spread(weights, rows_first):
    first, second = weights.shape
    rows, cols = (second, first) if rows_first else (first, second)
    pick = one_hot(rows * SUB, rows, lambda r: r // SUB, lambda c: c).astype(F32).astype(BF16)
    lay = one_hot(cols * SUB, cols, lambda r: r // SUB, lambda c: c).astype(F32).astype(BF16)
    same = one_hot(rows * SUB, cols * SUB, lambda r: r % SUB, lambda c: c % SUB)
    result = []
    for part in halves(weights):
        tall = mul(pick, part, NT if rows_first else NN).astype(BF16)
        wide = mul(tall, lay, NT)
        result.append(jnp.where(same, wide, 0.0).astype(BF16))
    return result


class Place:
    def __init__(self, px, py):
        self.px, self.py = px, py
        self.p = lax.axis_index("px")
        self.q = lax.axis_index("py")
        self.core = lax.rem(self.q, 2)
        self.side = self.q // 2
        self.mate = {"py": self.q + 1 - 2 * self.core}
        self.cross = {"py": lax.rem(self.q + 2, py)}

    def row_peer(self, step):
        return lax.rem(self.p + step, self.px)

    def col_peer(self, step):
        return lax.rem(self.q + step, self.py)

    def greet(self):
        barrier = pltpu.get_barrier_semaphore()
        for step in range(1, self.px):
            pl.semaphore_signal(barrier, inc=1, device_id={"px": self.row_peer(step)}, device_id_type=MESH)
        for step in range(1, self.py):
            pl.semaphore_signal(barrier, inc=1, device_id={"py": self.col_peer(step)}, device_id_type=MESH)
        pl.semaphore_wait(barrier, self.px + self.py - 2)


def remote(src, dst, send, recv, device):
    return pltpu.make_async_remote_copy(
        src_ref=src, dst_ref=dst, send_sem=send, recv_sem=recv, device_id=device, device_id_type=MESH,
    )


def forward_kernel(px, py, flow_ref, cot_ref, ty_ref, win_ref, wout_ref, tz_ref, tx_ref, out_ref,
                   tile, kron, lines_h, lines_l, modes_h, modes_l, ty, summed, from_mate, to_cross,
                   from_cross, to_row, gathered, load_sem, table_sem, mate_send, mate_recv,
                   cross_send, cross_recv, row_send, row_recv):
    here = Place(px, py)
    steps, channels, group, cols, depth = tile.shape
    tiles = steps // 2
    ranks = win_ref.shape[1]
    packs = ranks // 4
    loads = []
    for t in range(steps):
        source = flow_ref if t < tiles else cot_ref
        loads.append(pltpu.make_async_copy(
            source.at[:, pl.ds((t % tiles) * group, group)], tile.at[t], load_sem.at[t]))
        loads[t].start()
    table = pltpu.make_async_copy(ty_ref.at[here.q], ty, table_sem)
    table.start()
    here.greet()
    for f, weight in enumerate((win_ref, wout_ref)):
        high, low = spread(weight[...], True)
        kron[f, :ranks * SUB] = high
        kron[f, ranks * SUB:] = low
    table.wait()

    def mate_copies(t):
        return [remote(summed.at[t, 2 * s + 1 - here.core], from_mate.at[t, s],
                       mate_send.at[t, s], mate_recv.at[t, s], here.mate) for s in range(2)]

    def cross_copy(t):
        return remote(to_cross.at[t], from_cross.at[t], cross_send.at[t], cross_recv.at[t], here.cross)

    def row_copy(t, step):
        return remote(to_row.at[t, here.row_peer(step)], gathered.at[t // tiles, here.p, lax.rem(t, tiles)],
                      row_send.at[t, step], row_recv.at[t, step], {"px": here.row_peer(step)})

    def compute(t):
        f = t // tiles

        def lift(x, carry):
            sides = [tile[t, :, x, h * SUB:(h + 1) * SUB, :].reshape(channels * SUB, depth)
                     for h in range(cols // SUB)]
            both = mul(kron[f], jnp.concatenate(sides, axis=1))
            high, low = halves(both[:ranks * SUB] + both[ranks * SUB:])
            for a in range(ranks):
                for h in range(cols // SUB):
                    row = pl.multiple_of(x * (packs * cols) + (a // 4) * cols + h * SUB, SUB)
                    spot = (pl.ds(row, SUB), slice((a % 4) * depth, (a % 4 + 1) * depth))
                    part = (slice(a * SUB, (a + 1) * SUB), slice(h * depth, (h + 1) * depth))
                    lines_h[spot] = high[part]
                    lines_l[spot] = low[part]
            return carry

        lax.fori_loop(0, group, lift, 0)
        modes = mul3((lines_h[...], lines_l[...]), (tz_ref[0], tz_ref[1]))
        high, low = halves(modes)
        for x in range(group):
            for a in range(packs):
                for p in range(2):
                    spot = (slice((x * 2 + p) * cols, (x * 2 + p + 1) * cols), slice(a * LANES, (a + 1) * LANES))
                    part = (slice((x * packs + a) * cols, (x * packs + a + 1) * cols),
                            slice(p * LANES, (p + 1) * LANES))
                    modes_h[spot] = high[part]
                    modes_l[spot] = low[part]
        total = mul3((ty[0], ty[1]), (modes_h[...], modes_l[...]))
        summed[t] = total.reshape(summed.shape[1:])

    def body(t, carry):
        @pl.when(t < steps)
        def _():
            pltpu.make_async_copy(flow_ref.at[:, pl.ds(0, group)], tile.at[t], load_sem.at[t]).wait()
            compute(t)
            for copy in mate_copies(t):
                copy.start()

        @pl.when((t >= 1) & (t < steps + 1))
        def _():
            u = t - 1
            for copy in mate_copies(u):
                copy.wait_recv()
            to_cross[u] = summed[u, 2 * (1 - here.side) + here.core] + from_mate[u, 1 - here.side]
            cross_copy(u).start()

        @pl.when(t >= 3)
        def _():
            u = t - 3
            cross_copy(u).wait_recv()
            whole = summed[u, 2 * here.side + here.core] + from_mate[u, here.side] + from_cross[u]
            to_row[u] = whole
            for step in range(1, px):
                row_copy(u, step).start()
            gathered[u // tiles, here.p, lax.rem(u, tiles)] = to_row[u, here.p]

        return carry

    lax.fori_loop(0, steps + 3, body, 0)
    for f in range(2):
        for t in range(f * tiles, (f + 1) * tiles):
            for step in range(1, px):
                row_copy(t, step).wait_recv()
        lines = gathered[f].reshape(-1, packs * LANES)
        out_ref[f] = mul3((tx_ref[0], tx_ref[1]), halves(lines))

    def drain(t, carry):
        for copy in mate_copies(t):
            copy.wait_send()
        cross_copy(t).wait_send()
        for step in range(1, px):
            row_copy(t, step).wait_send()
        return carry

    lax.fori_loop(0, steps, drain, 0)


def mix_kernel(px, py, second_smem, spectra_ref, core_ref, first_ref, third_ref, scale_ref,
               mixed_ref, part_ref, small_ref, bk_ref, gk_ref, kernel_rows):
    k = lax.axis_index("py") * px + lax.axis_index("px")
    r2, rows, width = core_ref.shape
    m1, r1 = first_ref.shape
    m3, r3 = third_ref.shape
    packs = spectra_ref.shape[2] // LANES
    ranks = 4 * packs
    core = second_smem[k, 0] * core_ref[0]
    for s in range(1, r2):
        core = core + second_smem[k, s] * core_ref[s]
    pick = one_hot(width, r3, lambda r: r % r3, lambda c: c).astype(F32)
    small = exact(pick, third_ref[...], NT)
    wide = jnp.concatenate([small] * 4, axis=1)
    same = one_hot(width, LANES, lambda r: r // r3, lambda c: c // m3)
    third = jnp.where(same, wide, 0.0)
    heavy = exact(core, third)
    kernel_rows[...] = heavy
    group_of = iota((m1, LANES), 1) // m3
    columns = [jnp.broadcast_to(first_ref[:, r:r + 1], (m1, LANES)) for r in range(r1)]
    lift = [[spectra_ref[0, p * m1:(p + 1) * m1, a * LANES:(a + 1) * LANES] for a in range(packs)]
            for p in range(2)]
    scale = scale_ref[...]
    for p in range(2):
        for a in range(packs):
            bk_ref[p, a] = spectra_ref[1, p * m1:(p + 1) * m1, a * LANES:(a + 1) * LANES] * scale
    mixed_ref[...] = jnp.zeros_like(mixed_ref)

    def around(v):
        v = v + pltpu.roll(v, 64, 1)
        return v + pltpu.roll(v, 32, 1)

    def body(b, carry):
        mine = group_of == lax.rem(b, 4)
        kern = []
        for a in range(packs):
            block = kernel_rows[pl.ds(pl.multiple_of((b * packs + a) * r1, r1), r1), :]
            total = columns[0] * block[0:1]
            for r in range(1, r1):
                total = total + columns[r] * block[r:r + 1]
            kern.append(total)
        grad = [None] * packs
        for p in range(2):
            back = around(jnp.where(mine, bk_ref[p, b // 4], 0.0))
            sums = kern[0] * lift[p][0]
            for a in range(1, packs):
                sums = sums + kern[a] * lift[p][a]
            sums = jnp.where(mine, around(sums), 0.0)
            for a in range(packs):
                cell = (0, slice(p * m1, (p + 1) * m1), slice(a * LANES, (a + 1) * LANES))
                mixed_ref[cell] += kern[a] * back
                term = back * lift[p][a]
                grad[a] = term if p == 0 else grad[a] + term
            lanes = pl.ds(pl.multiple_of((b // 4) * LANES, LANES), LANES)
            mixed_ref[1, pl.ds(p * m1, m1), lanes] += sums
        for a in range(packs):
            gk_ref[:, pl.ds(pl.multiple_of((b * packs + a) * LANES, LANES), LANES)] = grad[a]
        return carry

    lax.fori_loop(0, ranks, body, 0)
    for p in range(2):
        for a in range(packs):
            cell = (1, slice(p * m1, (p + 1) * m1), slice(a * LANES, (a + 1) * LANES))
            mixed_ref[cell] = mixed_ref[cell] * scale
    count = rows // r1
    grads = gk_ref[...]
    spread_rows = jnp.concatenate([heavy[i * r1:(i + 1) * r1] for i in range(count)], axis=1)
    grad_first = exact(grads, spread_rows, NT)
    thin = exact(first_ref[...], grads, TN)
    tall = jnp.concatenate([thin[:, i * LANES:(i + 1) * LANES] for i in range(count)], axis=0)
    lay = one_hot(LANES, r3, lambda r: r % r3, lambda c: c).astype(F32)
    tiled = jnp.concatenate([third_ref[...]] * 4, axis=0)
    square = exact(tiled, lay, NT)
    match = one_hot(LANES, LANES, lambda r: r // m3, lambda c: (c // r3) % 4)
    part = exact(tall, jnp.where(match, square, 0.0))
    part_ref[...] = part
    cross = exact(tall, core, TN)
    cross = jnp.where(one_hot(LANES, width, lambda r: r // m3, lambda c: c // r3), cross, 0.0)
    cross = cross[:m3] + cross[m3:2 * m3] + cross[2 * m3:3 * m3] + cross[3 * m3:]
    shift = one_hot(width, LANES, lambda r: r % r3 + r1, lambda c: c).astype(F32)
    total = exact(cross, shift)
    total = total + exact(grad_first, one_hot(r1, LANES, lambda r: r, lambda c: c).astype(F32))
    lane = iota((m3, LANES), 1)
    row = iota((m3, LANES), 0)
    for s in range(r2):
        value = jnp.sum(core_ref[s] * part[:, :width])
        total = total + jnp.where((lane == r1 + r3 + s) & (row == k), value, 0.0)
    small_ref[...] = total


def backward_kernel(px, py, flow_ref, cot_ref, ty_ref, modes_ref, part_ref, small_ref, second_ref,
                    wout_ref, tx_ref, tz_ref, out_ref, core_out, small_out, pair_out,
                    tile, kron, to_row, blocks, ty, lines_h, lines_l, real_h, real_l, field, totals,
                    ranks_in, ranks_sum, ranks_col, core_all, small_row, small_sum, small_col,
                    pair_row, pair_sum, pair_col,
                    load_sem, table_sem, out_sem, row_send, row_recv, cross_send, cross_recv,
                    mate_send, mate_recv, rs_send, rs_recv, cs_send, cs_recv, ag_send, ag_recv,
                    bg_send, bg_recv, sr_send, sr_recv, sc_send, sc_recv, pr_send, pr_recv, pc_send, pc_recv):
    here = Place(px, py)
    steps, channels, group, cols, depth = tile.shape
    tiles = steps // 2
    ranks = wout_ref.shape[1]
    packs = ranks // 4
    q, p = here.q, here.p
    for t in range(steps):
        source = flow_ref if t < tiles else cot_ref
        pltpu.make_async_copy(
            source.at[:, pl.ds((t % tiles) * group, group)], tile.at[t], load_sem.at[t]).start()
    table = pltpu.make_async_copy(ty_ref.at[here.q], ty, table_sem)
    table.start()
    here.greet()
    share = part_ref.shape[0] // px
    piece = share // py

    def rs_copy(step):
        to = here.row_peer(step)
        return remote(part_ref.at[pl.ds(to * share, share)], ranks_in.at[p], rs_send.at[step], rs_recv.at[step],
                      {"px": to})

    def cs_copy(step):
        to = here.col_peer(step)
        return remote(ranks_sum.at[to], ranks_col.at[q], cs_send.at[step], cs_recv.at[step], {"py": to})

    def ag_copy(step):
        return remote(core_all.at[p, q], core_all.at[p, q], ag_send.at[step], ag_recv.at[step],
                      {"px": here.row_peer(step)})

    def bg_copy(step):
        return remote(core_all.at[:, q], core_all.at[:, q], bg_send.at[step], bg_recv.at[step],
                      {"py": here.col_peer(step)})

    def sr_copy(step):
        return remote(small_ref, small_row.at[p], sr_send.at[step], sr_recv.at[step],
                      {"px": here.row_peer(step)})

    def sc_copy(step):
        return remote(small_sum, small_col.at[q], sc_send.at[step], sc_recv.at[step],
                      {"py": here.col_peer(step)})

    def pr_copy(step):
        return remote(pair_sum.at[0], pair_row.at[p], pr_send.at[step], pr_recv.at[step],
                      {"px": here.row_peer(step)})

    def pc_copy(step):
        return remote(pair_sum.at[1], pair_col.at[q], pc_send.at[step], pc_recv.at[step],
                      {"py": here.col_peer(step)})

    def row_copy(t, step):
        to = here.row_peer(step)
        return remote(to_row.at[t // tiles, to, lax.rem(t, tiles)], blocks.at[t, q, p],
                      row_send.at[t, step], row_recv.at[t, step], {"px": to})

    def cross_copy(t):
        return remote(blocks.at[t, q], blocks.at[t, q], cross_send.at[t], cross_recv.at[t], here.cross)

    def mate_copy(t, s):
        quarter = q if s == 0 else lax.rem(q + 2, py)
        return remote(blocks.at[t, quarter], blocks.at[t, quarter],
                      mate_send.at[t, s], mate_recv.at[t, s], here.mate)

    for f in range(2):
        lines = mul3((tx_ref[0], tx_ref[1]), halves(modes_ref[f]))
        to_row[f] = lines.reshape(to_row.shape[1:])
        for t in range(f * tiles, (f + 1) * tiles):
            for step in range(1, px):
                row_copy(t, step).start()
            blocks[t, q, p] = to_row[f, p, t - f * tiles]
    for step in range(1, px):
        rs_copy(step).start()
        sr_copy(step).start()
    ranks_in[p] = part_ref[pl.ds(pl.multiple_of(p * share, share), share), :]
    small_row[p] = small_ref[...]
    high, low = spread(wout_ref[...], False)
    kron[0] = high
    kron[1] = low
    totals[...] = jnp.zeros_like(totals)
    table.wait()

    def place(t):
        high, low = halves(blocks[t].reshape(-1, packs * LANES))
        modes = mul3((ty[0], ty[1]), (high, low))
        high, low = halves(modes)
        for x in range(group):
            for a in range(packs):
                for o in range(2):
                    part = (slice((x * 2 + o) * cols, (x * 2 + o + 1) * cols), slice(a * LANES, (a + 1) * LANES))
                    spot = (slice((x * packs + a) * cols, (x * packs + a + 1) * cols),
                            slice(o * LANES, (o + 1) * LANES))
                    lines_h[spot] = high[part]
                    lines_l[spot] = low[part]
        real = mul3((lines_h[...], lines_l[...]), (tz_ref[0], tz_ref[1]))
        high, low = halves(real)
        for x in range(group):
            for a in range(ranks):
                for h in range(cols // SUB):
                    row = (x * packs + a // 4) * cols + h * SUB
                    part = (slice(row, row + SUB), slice((a % 4) * depth, (a % 4 + 1) * depth))
                    spot = (x, slice(a * SUB, (a + 1) * SUB), slice(h * depth, (h + 1) * depth))
                    real_h[spot] = high[part]
                    real_l[spot] = low[part]

    def outer(t):
        def one(x, carry):
            sides = [tile[t, :, x, h * SUB:(h + 1) * SUB, :].reshape(channels * SUB, depth)
                     for h in range(cols // SUB)]
            cells = jnp.concatenate(sides, axis=1)
            totals[t // tiles] += mul(cells, real_h[x], NT) + mul(cells, real_l[x], NT)
            return carry

        lax.fori_loop(0, group, one, 0)

    def emit(t):
        g = t - tiles

        def one(x, carry):
            both = mul3((kron[0], kron[1]), (real_h[x], real_l[x])).astype(BF16)
            for h in range(cols // SUB):
                field[g, :, x, h * SUB:(h + 1) * SUB, :] = both[:, h * depth:(h + 1) * depth].reshape(
                    channels, SUB, depth)
            return carry

        lax.fori_loop(0, group, one, 0)
        out_copy(g).start()

    def out_copy(g):
        return pltpu.make_async_copy(field.at[g], out_ref.at[:, pl.ds(g * group, group)], out_sem.at[g])

    def body(i, carry):
        @pl.when(i < steps)
        def _():
            for step in range(1, px):
                row_copy(i, step).wait_recv()
            cross_copy(i).start()
            mate_copy(i, 0).start()

        @pl.when((i >= 2) & (i < steps + 2))
        def _():
            cross_copy(i - 2).wait_recv()
            mate_copy(i - 2, 1).start()

        @pl.when(i >= 3)
        def _():
            t = i - 3
            for s in range(2):
                mate_copy(t, s).wait_recv()
            pltpu.make_async_copy(flow_ref.at[:, pl.ds(0, group)], tile.at[t], load_sem.at[t]).wait()
            place(t)
            outer(t)

        @pl.when(i >= 3 + tiles)
        def _():
            emit(i - 3)

        @pl.when(i == 4)
        def _():
            for step in range(1, px):
                rs_copy(step).wait_recv()
                sr_copy(step).wait_recv()
            half = second_ref.shape[2] // LANES
            mine = second_ref[q]
            sums = []
            for o in range(half):
                total = None
                for s in range(px):
                    weight = mine[s:s + 1, o * LANES:(o + 1) * LANES]
                    term = ranks_in[s] * weight
                    total = term if total is None else total + term
                sums.append(total)
            ranks_sum[...] = jnp.concatenate(sums, axis=1).reshape(ranks_sum.shape)
            total = small_row[0]
            for s in range(1, px):
                total = total + small_row[s]
            small_sum[...] = total
            small_col[q] = total
            ranks_col[q] = ranks_sum[q]
            for step in range(1, py):
                cs_copy(step).start()
                sc_copy(step).start()

        @pl.when(i == 6)
        def _():
            for step in range(1, py):
                cs_copy(step).wait_recv()
                sc_copy(step).wait_recv()
            total = ranks_col[0]
            small = small_col[0]
            for s in range(1, py):
                total = total + ranks_col[s]
                small = small + small_col[s]
            core_all[p, q] = total
            small_out[...] = small
            for step in range(1, px):
                ag_copy(step).start()

        @pl.when(i == 8)
        def _():
            for step in range(1, px):
                ag_copy(step).wait_recv()
            for step in range(1, py):
                bg_copy(step).start()

        return carry

    lax.fori_loop(0, steps + 3, body, 0)
    keep = one_hot(channels * SUB, ranks * SUB, lambda r: r % SUB, lambda c: c % SUB)
    pair = None
    for f in range(2):
        grid = jnp.where(keep, totals[f], 0.0).reshape(channels, SUB, ranks * SUB).sum(axis=1)
        for i in range(channels // SUB):
            base = (2 * i + f) * ranks
            pick = one_hot(ranks * SUB, LANES, lambda r: r // SUB + base, lambda c: c).astype(F32)
            term = exact(grid[i * SUB:(i + 1) * SUB], pick)
            pair = term if pair is None else pair + term
    pair_sum[0] = pair
    pair_row[p] = pair
    for step in range(1, px):
        pr_copy(step).start()
    for step in range(1, py):
        bg_copy(step).wait_recv()
    core_out[...] = core_all[...]
    for step in range(1, px):
        pr_copy(step).wait_recv()
    total = pair_row[0]
    for s in range(1, px):
        total = total + pair_row[s]
    pair_sum[1] = total
    pair_col[q] = total
    for step in range(1, py):
        pc_copy(step).start()
    for step in range(1, py):
        pc_copy(step).wait_recv()
    total = pair_col[0]
    for s in range(1, py):
        total = total + pair_col[s]
    pair_out[...] = total

    def drain(t, carry):
        for step in range(1, px):
            row_copy(t, step).wait_send()
        cross_copy(t).wait_send()
        for s in range(2):
            mate_copy(t, s).wait_send()
        return carry

    lax.fori_loop(0, steps, drain, 0)
    for step in range(1, px):
        for copy in (rs_copy, sr_copy, ag_copy, pr_copy):
            copy(step).wait_send()
    for step in range(1, py):
        for copy in (cs_copy, sc_copy, bg_copy, pc_copy):
            copy(step).wait_send()
    for g in range(tiles):
        out_copy(g).wait()


def fast_shards(px, py, flow_field, cotangent, tucker_core, in_factor, out_factor,
                first_factor, second_factor, third_factor):
    channels, rows, cols, depth = flow_field.shape
    ri, ro, r1, r2, r3 = tucker_core.shape
    group = 2 * LANES // (2 * cols)
    tiles = rows // group
    steps = 2 * tiles
    packs = ri // 4
    wide = packs * LANES
    keep = px
    inverse_count = 1.0 / (NX * NY * NZ)

    small = np_depth(NZ, M3)
    tz = np.einsum("st,pzm->szptm", np.eye(4), small).reshape(4 * depth, 2 * 4 * M3)
    turn = np_turn(M2, NY).reshape(2, py, cols, 2, py, keep)
    ty = np.einsum("pdyoqk,xw->dqkxowpy", turn, np.eye(group))
    ty = ty.reshape(py, py * keep * group * 2, group * 2 * cols)
    turn = np_turn(M1, NX).reshape(2, NX, 2, M1)
    tx = turn.transpose(2, 3, 1, 0).reshape(2 * M1, NX * 2)
    tz_f, tz_b = np_halves(tz), np_halves(tz.T)
    ty_f = np_halves(ty).swapaxes(0, 1)
    ty_b = np_halves(ty.swapaxes(1, 2)).swapaxes(0, 1)
    tx_f, tx_b = np_halves(tx), np_halves(tx.T)
    weight = np.where(np.arange(M3) == 0, 1.0, 2.0) * inverse_count
    scale = jnp.asarray(np.tile(weight, 4)[None, :].astype(np.float32))

    vmem = pl.BlockSpec(memory_space=pltpu.VMEM)
    anywhere = pl.BlockSpec(memory_space=pl.ANY)
    shape = jax.ShapeDtypeStruct
    dma = pltpu.SemaphoreType.DMA

    def params(number):
        return pltpu.CompilerParams(
            vmem_limit_bytes=VMEM_LIMIT, collective_id=number, has_side_effects=True)

    def cost(flops):
        return pl.CostEstimate(flops=flops, bytes_accessed=10 ** 7, transcendentals=0)

    lines = group * packs * cols
    block = (keep, 2 * group, wide)
    spectra = pl.pallas_call(
        functools.partial(forward_kernel, px, py),
        out_shape=shape((2, 2 * M1, wide), F32),
        in_specs=[anywhere, anywhere, anywhere, vmem, vmem, vmem, vmem],
        out_specs=vmem,
        scratch_shapes=[
            pltpu.VMEM((steps, channels, group, cols, depth), BF16),
            pltpu.VMEM((2, 2 * ri * SUB, channels * SUB), BF16),
            pltpu.VMEM((lines, 4 * depth), BF16), pltpu.VMEM((lines, 4 * depth), BF16),
            pltpu.VMEM((group * 2 * cols, wide), BF16), pltpu.VMEM((group * 2 * cols, wide), BF16),
            pltpu.VMEM(ty_f.shape[1:], BF16),
            pltpu.VMEM((steps, py) + block, F32),
            pltpu.VMEM((steps, 2) + block, F32),
            pltpu.VMEM((steps,) + block, F32),
            pltpu.VMEM((steps,) + block, F32),
            pltpu.VMEM((steps,) + block, F32),
            pltpu.VMEM((2, px, tiles, 2 * group, wide), F32),
            dma((steps,)), dma,
            dma((steps, 2)), dma((steps, 2)), dma((steps,)), dma((steps,)),
            dma((steps, px)), dma((steps, px)),
        ],
        compiler_params=params(0), cost_estimate=cost(10 ** 10),
    )(flow_field, cotangent, jnp.asarray(ty_f), in_factor, out_factor, jnp.asarray(tz_f), jnp.asarray(tx_f))

    core = tucker_core.reshape(packs, 4, ro, r1, r2, r3).transpose(4, 2, 0, 3, 1, 5)
    core = core.reshape(r2, ro * packs * r1, 4 * r3)
    count = ro * packs * r1
    smem = pl.BlockSpec(memory_space=pltpu.SMEM)
    modes, part, little = pl.pallas_call(
        functools.partial(mix_kernel, px, py),
        out_shape=(shape((2, 2 * M1, wide), F32), shape((count, LANES), F32), shape((M3, LANES), F32)),
        in_specs=[smem, vmem, vmem, vmem, vmem, vmem], out_specs=(vmem,) * 3,
        scratch_shapes=[
            pltpu.VMEM((2, packs, M1, LANES), F32),
            pltpu.VMEM((M1, ro * wide), F32),
            pltpu.VMEM((count, LANES), F32),
        ],
        compiler_params=pltpu.CompilerParams(vmem_limit_bytes=VMEM_LIMIT), cost_estimate=cost(10 ** 9),
    )(second_factor, spectra, core, first_factor, third_factor, scale)

    spread_second = jnp.repeat(second_factor, LANES // 4, axis=1).reshape(py, px, -1)
    share, piece = count // px, count // px // py
    span = spread_second.shape[2]
    out, core_sum, little, pair = pl.pallas_call(
        functools.partial(backward_kernel, px, py),
        out_shape=(
            shape(flow_field.shape, BF16), shape((px, py, piece, span), F32),
            shape((M3, LANES), F32), shape((SUB, LANES), F32),
        ),
        in_specs=[anywhere, anywhere, anywhere] + [vmem] * 7,
        out_specs=(anywhere, vmem, vmem, vmem),
        scratch_shapes=[
            pltpu.VMEM((steps, channels, group, cols, depth), BF16),
            pltpu.VMEM((2, channels * SUB, ro * SUB), BF16),
            pltpu.VMEM((2, px, tiles, 2 * group, wide), F32),
            pltpu.VMEM((steps, py) + block, F32),
            pltpu.VMEM(ty_b.shape[1:], BF16),
            pltpu.VMEM((lines, 2 * LANES), BF16), pltpu.VMEM((lines, 2 * LANES), BF16),
            pltpu.VMEM((group, ri * SUB, cols // SUB * depth), BF16),
            pltpu.VMEM((group, ri * SUB, cols // SUB * depth), BF16),
            pltpu.VMEM((tiles, channels, group, cols, depth), BF16),
            pltpu.VMEM((2, channels * SUB, ri * SUB), F32),
            pltpu.VMEM((px, share, LANES), F32), pltpu.VMEM((py, piece, span), F32),
            pltpu.VMEM((py, piece, span), F32), pltpu.VMEM((px, py, piece, span), F32),
            pltpu.VMEM((px, M3, LANES), F32), pltpu.VMEM((M3, LANES), F32), pltpu.VMEM((py, M3, LANES), F32),
            pltpu.VMEM((px, SUB, LANES), F32), pltpu.VMEM((2, SUB, LANES), F32), pltpu.VMEM((py, SUB, LANES), F32),
            dma((steps,)), dma, dma((tiles,)),
            dma((steps, px)), dma((steps, px)), dma((steps,)), dma((steps,)),
            dma((steps, 2)), dma((steps, 2)),
            dma((px,)), dma((px,)), dma((py,)), dma((py,)), dma((px,)), dma((px,)), dma((py,)), dma((py,)),
            dma((px,)), dma((px,)), dma((py,)), dma((py,)), dma((px,)), dma((px,)), dma((py,)), dma((py,)),
        ],
        compiler_params=params(1), cost_estimate=cost(10 ** 10),
    )(flow_field, cotangent, jnp.asarray(ty_b), modes, part, little, spread_second, out_factor,
      jnp.asarray(tx_b), jnp.asarray(tz_b))

    core_grad = core_sum.reshape(ro, packs, r1, r2, 4, r3).transpose(1, 4, 0, 2, 3, 5).reshape(tucker_core.shape)
    pair = pair.reshape(SUB, channels // SUB, 2, ri).transpose(2, 1, 0, 3).reshape(2, channels, ri)
    return (out, core_grad, pair[0], pair[1], little[:, :r1],
            little[:, r1 + r3:r1 + r3 + r2], little[:, r1:r1 + r3])


def solution(mesh):
    px, py = mesh.shape["px"], mesh.shape["py"]
    rows, cols = NX // px, NY // py
    fits = py == 4 and px * py == M2 and cols == 32 and rows % 4 == 0 and NZ == LANES
    fits = fits and M1 == 32 and M3 == 32
    body = functools.partial(fast_shards, px, py) if fits else shards
    return jax.shard_map(
        body,
        mesh=mesh,
        in_specs=(
            P(None, "px", "py", None),
            P(None, "px", "py", None),
            P(),
            P(),
            P(),
            P(),
            P(),
            P(),
        ),
        out_specs=(P(None, "px", "py", None), P(), P(), P(), P(), P(), P()),
        check_vma=False,
    )
```

```python
import functools
import math

import jax
import jax.numpy as jnp
import numpy as np
from jax import lax
from jax.experimental import pallas as pl
from jax.experimental.pallas import tpu as pltpu
from jax.sharding import PartitionSpec as P

NX = 128
NY = 128
NZ = 128
M1 = 32
M2 = 32
M3 = 32


HIGHEST = lax.Precision.HIGHEST


def turn_table(count, length):
    position = jnp.arange(count)
    frequency = jnp.where(position < count // 2, position, position - count)
    cells_at = jnp.arange(length)
    phase = frequency[None, :] * cells_at[:, None] % length
    angle = 2.0 * math.pi / length * phase.astype(jnp.float32)
    cosine = jnp.cos(angle)
    sine = jnp.sin(angle)
    upper = jnp.stack([cosine, -sine], axis=1)
    lower = jnp.stack([sine, cosine], axis=1)
    return jnp.stack([upper, lower])


def depth_table(length, count):
    cells_at = jnp.arange(length)
    frequency = jnp.arange(count)
    phase = cells_at[:, None] * frequency[None, :] % length
    angle = 2.0 * math.pi / length * phase.astype(jnp.float32)
    return jnp.concatenate([jnp.cos(angle), -jnp.sin(angle)], axis=1)


def to_modes(fields, depth_tables):
    across = turn_table(M2, NY)
    along = turn_table(M1, NX)
    spectra = []
    for member, z_table in zip(fields, depth_tables):
        channels, rows_here, cols_here, depth_len = member.shape
        flat = jnp.dot(member.reshape(-1, depth_len), z_table, precision=HIGHEST)
        spectra.append(flat.reshape(channels, rows_here, cols_here, 2, M3))
    members = lax.all_to_all(tuple(spectra), "py", split_axis=4, concat_axis=2, tiled=True)
    lines = tuple(
        (jnp.einsum("cxypm,pyqk->cxqkm", member, across, precision=HIGHEST) for member in members)
    )
    members = (
        lax.all_to_all(lines[0], "px", split_axis=3, concat_axis=1, tiled=True),
        lax.all_to_all(lines[1], "px", split_axis=3, concat_axis=1, tiled=True),
    )
    return tuple(
        (jnp.einsum("cxpkm,pxqj->cqjkm", member, along, precision=HIGHEST) for member in members)
    )


def to_space(modes, depth_weights):
    across = turn_table(M2, NY)
    along = turn_table(M1, NX)
    depth_base = depth_table(NZ, M3).T.reshape(2, M3, NZ)
    lines = tuple(
        (jnp.einsum("cqjkm,pxqj->cpxkm", member, along, precision=HIGHEST) for member in modes)
    )
    members = (
        lax.all_to_all(lines[0], "px", split_axis=2, concat_axis=3, tiled=True),
        lax.all_to_all(lines[1], "px", split_axis=2, concat_axis=3, tiled=True),
    )
    columns = tuple(
        (jnp.einsum("cqxkm,pyqk->cpxym", member, across, precision=HIGHEST) for member in members)
    )
    members = (
        lax.all_to_all(columns[0], "py", split_axis=3, concat_axis=4, tiled=True),
        lax.all_to_all(columns[1], "py", split_axis=3, concat_axis=4, tiled=True),
    )
    return tuple(
        (
            jnp.einsum(
                "cpxyk,pkn->cxyn", member, depth_base * weight_row[None, :, None], precision=HIGHEST
            )
            for member, weight_row in zip(members, depth_weights)
        )
    )


def shards(
    flow_field,
    cotangent,
    tucker_core,
    in_factor,
    out_factor,
    first_factor,
    second_factor,
    third_factor,
):
    inverse_count = 1.0 / (NX * NY * NZ)
    weights = jnp.where(jnp.arange(M3) == 0, 1.0, 2.0).astype(jnp.float32)
    unit_weights = jnp.ones((M3,), jnp.float32)
    base_table = depth_table(NZ, M3)
    weighted_table = base_table * jnp.concatenate([weights, weights])[None, :]
    block_second = M2 // lax.axis_size("px")
    block_third = M3 // lax.axis_size("py")
    start_second = lax.axis_index("px") * block_second
    start_third = lax.axis_index("py") * block_third

    def build_kernel(core_arg, first_arg, second_arg, third_arg):
        second_rows = lax.dynamic_slice_in_dim(second_arg, start_second, block_second, 0)
        third_rows = lax.dynamic_slice_in_dim(third_arg, start_third, block_third, 0)
        partial_core = jnp.einsum("abrst,mt->abrsm", core_arg, third_rows, precision=HIGHEST)
        partial_core = jnp.einsum("abrsm,ks->abrkm", partial_core, second_rows, precision=HIGHEST)
        return jnp.einsum("abrkm,jr->abjkm", partial_core, first_arg, precision=HIGHEST)

    kernel, pullback = jax.vjp(build_kernel, tucker_core, first_factor, second_factor, third_factor)
    field_wide = flow_field.astype(jnp.float32)
    back_wide = cotangent.astype(jnp.float32)
    lifted_grid = jnp.einsum("cxyn,ca->axyn", field_wide, in_factor, precision=HIGHEST)
    back_grid = jnp.einsum("cxyn,cb->bxyn", back_wide, out_factor, precision=HIGHEST)
    lifted, back_mixed = to_modes((lifted_grid, back_grid), (base_table, weighted_table))
    back_mixed = back_mixed * inverse_count
    mixed = jnp.einsum("abjkm,apjkm->bpjkm", kernel, lifted, precision=HIGHEST)
    grad_kernel = jnp.einsum("bpjkm,apjkm->abjkm", back_mixed, lifted, precision=HIGHEST)
    back_lifted = jnp.einsum("abjkm,bpjkm->apjkm", kernel, back_mixed, precision=HIGHEST)
    mixed_grid, lifted_back = to_space((mixed, back_lifted), (weights, unit_weights))
    mixed_grid = mixed_grid * inverse_count
    output_field = jnp.einsum("ob,bxyn->oxyn", out_factor, mixed_grid, precision=HIGHEST).astype(
        jnp.bfloat16
    )
    grad_out = jnp.einsum("oxyn,bxyn->ob", back_wide, mixed_grid, precision=HIGHEST)
    grad_in = jnp.einsum("ixyn,axyn->ia", field_wide, lifted_back, precision=HIGHEST)
    grad_core, grad_first, grad_second, grad_third = pullback(grad_kernel)
    totals = lax.psum(
        (grad_core, grad_in, grad_out, grad_first, grad_second, grad_third), ("px", "py")
    )
    return (output_field, totals[0], totals[1], totals[2], totals[3], totals[4], totals[5])


BF16 = jnp.bfloat16
F32 = jnp.float32
NN = (((1,), (0,)), ((), ()))
NT = (((1,), (1,)), ((), ()))
TN = (((0,), (0,)), ((), ()))
MESH = pl.DeviceIdType.MESH
VMEM_LIMIT = 63 * 1024 * 1024
SUB = 16
LANES = 128


def mul(a, b, dims=NN):
    return lax.dot_general(a, b, dims, preferred_element_type=F32)


def exact(a, b, dims=NN):
    return lax.dot_general(a, b, dims, precision=HIGHEST, preferred_element_type=F32)


def halves(x):
    high = x.astype(BF16)
    return high, (x - high.astype(F32)).astype(BF16)


def mul3(a, b, dims=NN):
    (ah, al), (bh, bl) = a, b
    return mul(ah, bh, dims) + (mul(ah, bl, dims) + mul(al, bh, dims))


def np_halves(x):
    x = np.asarray(x, np.float32)
    high = x.astype(BF16)
    return np.stack([high, (x - high.astype(np.float32)).astype(BF16)])


def np_turn(count, length):
    position = np.arange(count)
    frequency = np.where(position < count // 2, position, position - count)
    phase = frequency[None, :] * np.arange(length)[:, None] % length
    angle = 2.0 * np.pi / length * phase
    upper = np.stack([np.cos(angle), -np.sin(angle)], axis=1)
    lower = np.stack([np.sin(angle), np.cos(angle)], axis=1)
    return np.stack([upper, lower])


def np_depth(length, count):
    phase = np.arange(length)[:, None] * np.arange(count)[None, :] % length
    angle = 2.0 * np.pi / length * phase
    return np.stack([np.cos(angle), -np.sin(angle)])


def iota(shape, axis):
    return lax.broadcasted_iota(jnp.int32, shape, axis)


def one_hot(rows, cols, row_of, col_of):
    return row_of(iota((rows, cols), 0)) == col_of(iota((rows, cols), 1))


def spread(weights, dims):
    rows, cols = weights.shape if dims == NN else weights.shape[::-1]
    pick = one_hot(rows * SUB, rows, lambda r: r // SUB, lambda c: c).astype(F32).astype(BF16)
    lay = one_hot(cols * SUB, cols, lambda r: r // SUB, lambda c: c).astype(F32).astype(BF16)
    same = one_hot(rows * SUB, cols * SUB, lambda r: r % SUB, lambda c: c % SUB)
    result = []
    for part in halves(weights):
        tall = mul(pick, part, dims).astype(BF16)
        wide = mul(tall, lay, NT)
        result.append(jnp.where(same, wide, 0.0).astype(BF16))
    return result


def unfold(row, count, width):
    tall = jnp.broadcast_to(row, (count, row.shape[1]))
    return pltpu.roll(tall, 0, 1, stride=width, stride_axis=0)


class Place:
    def __init__(self, px, py):
        self.px, self.py = px, py
        self.p = lax.axis_index("px")
        self.q = lax.axis_index("py")
        self.core = lax.rem(self.q, 2)
        self.side = self.q // 2
        self.mate = {"py": self.q + 1 - 2 * self.core}
        self.cross = {"py": lax.rem(self.q + 2, py)}

    def row_peer(self, step):
        return lax.rem(self.p + step, self.px)

    def col_peer(self, step):
        return lax.rem(self.q + step, self.py)

    def greet(self):
        barrier = pltpu.get_barrier_semaphore()
        for step in range(1, self.px):
            pl.semaphore_signal(barrier, inc=1, device_id={"px": self.row_peer(step)}, device_id_type=MESH)
        for step in range(1, self.py):
            pl.semaphore_signal(barrier, inc=1, device_id={"py": self.col_peer(step)}, device_id_type=MESH)

    def meet(self):
        pl.semaphore_wait(pltpu.get_barrier_semaphore(), self.px + self.py - 2)


def remote(src, dst, send, recv, device):
    return pltpu.make_async_remote_copy(
        src_ref=src, dst_ref=dst, send_sem=send, recv_sem=recv, device_id=device, device_id_type=MESH,
    )


def remote_kernel(px, py, second_ref, flow_ref, cot_ref, tyf_ref, tyb_ref, core_ref, win_ref, wout_ref,
                  first_ref, third_ref, scale_ref, tzf_ref, txf_ref, tzb_ref, txb_ref,
                  real_h_out, real_l_out, core_out, pack_out,
                  tile, kron, lines_h, lines_l, modes_h, modes_l, tyf, tyb, core, summed, from_mate, to_cross,
                  from_cross, to_row, gathered, lifted, backed, mixed, core_rows, kernel_rows, grads, back_row,
                  blocks, back_h, back_l, real_h, real_l, totals, partial, ranks_in, ranks_sum, ranks_col,
                  core_all, pack_sum, pack_row, pack_col,
                  load_sem, table_sem, mate_send, mate_recv, cross_send, cross_recv, row_send, row_recv,
                  brow_send, brow_recv, bcross_send, bcross_recv, bmate_send, bmate_recv, real_sem,
                  rs_send, rs_recv, cs_send, cs_recv, ag_send, ag_recv, bg_send, bg_recv,
                  pr_send, pr_recv, pc_send, pc_recv):
    here = Place(px, py)
    p, q = here.p, here.q
    k = q * px + p
    steps, channels, group, cols, depth = tile.shape
    tiles = steps // 2
    ranks = win_ref.shape[0]
    packs = ranks // 4
    r1, m1 = first_ref.shape
    r3, m3 = third_ref.shape
    r2 = second_ref.shape[0]
    wide = packs * LANES

    here.greet()
    for t in range(steps):
        source = flow_ref if t < tiles else cot_ref
        pltpu.make_async_copy(
            source.at[:, pl.ds((t % tiles) * group, group)], tile.at[t], load_sem.at[t]).start()
    tables = [pltpu.make_async_copy(tyf_ref.at[q], tyf, table_sem.at[0]),
              pltpu.make_async_copy(tyb_ref.at[q], tyb, table_sem.at[1]),
              pltpu.make_async_copy(core_ref, core, table_sem.at[2])]
    for copy in tables:
        copy.start()
    for f, weight in enumerate((win_ref, wout_ref)):
        high, low = spread(weight[...], NN)
        kron[f, :ranks * SUB] = high
        kron[f, ranks * SUB:] = low
    totals[...] = jnp.zeros_like(totals)
    tables[0].wait()

    def mate_copies(t):
        return [remote(summed.at[t, 2 * s + 1 - here.core], from_mate.at[t, s],
                       mate_send.at[t, s], mate_recv.at[t, s], here.mate) for s in range(2)]

    def cross_copy(t):
        return remote(to_cross.at[t], from_cross.at[t], cross_send.at[t], cross_recv.at[t], here.cross)

    def row_copy(t, step):
        return remote(to_row.at[t, here.row_peer(step)], gathered.at[t // tiles, p, lax.rem(t, tiles)],
                      row_send.at[t, step], row_recv.at[t, step], {"px": here.row_peer(step)})

    def compute(t):
        f = t // tiles

        def lift(x, carry):
            sides = [tile[t, :, x, h * SUB:(h + 1) * SUB, :].reshape(channels * SUB, depth)
                     for h in range(cols // SUB)]
            both = mul(kron[f], jnp.concatenate(sides, axis=1))
            high, low = halves(both[:ranks * SUB] + both[ranks * SUB:])
            for a in range(ranks):
                for h in range(cols // SUB):
                    row = pl.multiple_of(x * (packs * cols) + (a // 4) * cols + h * SUB, SUB)
                    spot = (pl.ds(row, SUB), slice((a % 4) * depth, (a % 4 + 1) * depth))
                    part = (slice(a * SUB, (a + 1) * SUB), slice(h * depth, (h + 1) * depth))
                    lines_h[spot] = high[part]
                    lines_l[spot] = low[part]
            return carry

        lax.fori_loop(0, group, lift, 0)
        modes = mul3((lines_h[...], lines_l[...]), (tzf_ref[0], tzf_ref[1]))
        high, low = halves(modes)
        for x in range(group):
            for a in range(packs):
                for o in range(2):
                    spot = (slice((x * 2 + o) * cols, (x * 2 + o + 1) * cols), slice(a * LANES, (a + 1) * LANES))
                    part = (slice((x * packs + a) * cols, (x * packs + a + 1) * cols),
                            slice(o * LANES, (o + 1) * LANES))
                    modes_h[spot] = high[part]
                    modes_l[spot] = low[part]
        total = mul3((tyf[0], tyf[1]), (modes_h[...], modes_l[...]))
        summed[t] = total.reshape(summed.shape[1:])

    def kernel_side():
        tables[2].wait()

        def one(a, carry):
            for r in range(r1):
                total = second_ref[0, k] * core[a, r, 0]
                for s in range(1, r2):
                    total = total + second_ref[s, k] * core[a, r, s]
                core_rows[pl.ds(pl.multiple_of((a * r1 + r) * r3, r3), r3), :ranks] = total
            return carry

        core_rows[...] = jnp.zeros_like(core_rows)
        lax.fori_loop(0, ranks, one, 0)
        kernel_rows[...] = exact(folded(), widen())

    def folded():
        total = core_rows[pl.ds(0, ranks * r1, stride=r3), :]
        for t in range(1, r3):
            total = total + pltpu.roll(core_rows[pl.ds(t, ranks * r1, stride=r3), :], (r3 - t) * ranks, 1)
        return total

    def widen():
        tall = one_hot(LANES, r3, lambda r: (r3 - r // ranks) % r3, lambda c: c).astype(F32)
        flat = one_hot(m3, wide, lambda r: r, lambda c: c % m3).astype(F32)
        full = exact(exact(tall, third_ref[...]), flat)
        return jnp.where(one_hot(LANES, wide, lambda r: r % ranks, lambda c: c // m3), full, 0.0)

    def body(t, carry):
        @pl.when(t < steps)
        def _():
            pltpu.make_async_copy(flow_ref.at[:, pl.ds(0, group)], tile.at[t], load_sem.at[t]).wait()
            compute(t)

        @pl.when(t == 0)
        def _():
            here.meet()

        @pl.when(t < steps)
        def _():
            for copy in mate_copies(t):
                copy.start()

        @pl.when((t >= 1) & (t < steps + 1))
        def _():
            u = t - 1
            for copy in mate_copies(u):
                copy.wait_recv()
            to_cross[u] = summed[u, 2 * (1 - here.side) + here.core] + from_mate[u, 1 - here.side]
            cross_copy(u).start()

        @pl.when(t == steps)
        def _():
            kernel_side()

        @pl.when(t >= 3)
        def _():
            u = t - 3
            cross_copy(u).wait_recv()
            to_row[u] = summed[u, 2 * here.side + here.core] + from_mate[u, here.side] + from_cross[u]
            for step in range(1, px):
                row_copy(u, step).start()
            gathered[u // tiles, p, lax.rem(u, tiles)] = to_row[u, p]

        return carry

    lax.fori_loop(0, steps + 3, body, 0)
    scale = scale_ref[...]
    for f in range(2):
        for t in range(f * tiles, (f + 1) * tiles):
            for step in range(1, px):
                row_copy(t, step).wait_recv()
        lines = mul3((txf_ref[0], txf_ref[1]), halves(gathered[f].reshape(-1, wide)))
        for o in range(2):
            for a in range(packs):
                cell = lines[o * m1:(o + 1) * m1, a * LANES:(a + 1) * LANES]
                if f == 0:
                    lifted[o, a] = cell
                else:
                    backed[o, a] = cell * scale

    group_of = iota((m1, LANES), 1) // m3
    lay = one_hot(r1 * LANES, r1, lambda r: r // LANES, lambda c: c).astype(F32)
    columns = exact(first_ref[...], lay, (((0,), (1,)), ((), ())))
    mixed[...] = jnp.zeros_like(mixed)

    def around(v):
        v = v + pltpu.roll(v, 64, 1)
        return v + pltpu.roll(v, 32, 1)

    def blend(a, carry):
        mine = group_of == lax.rem(a, 4)
        block = kernel_rows[pl.ds(pl.multiple_of(a * r1, r1), r1), :]
        kern = []
        for b in range(packs):
            total = columns[:, :LANES] * block[0:1, b * LANES:(b + 1) * LANES]
            for r in range(1, r1):
                total = total + columns[:, r * LANES:(r + 1) * LANES] * block[r:r + 1, b * LANES:(b + 1) * LANES]
            kern.append(total)
        grad = [None] * packs
        for o in range(2):
            lift = around(jnp.where(mine, lifted[o, a // 4], 0.0))
            sums = None
            for b in range(packs):
                back = backed[o, b]
                term = kern[b] * back
                sums = term if sums is None else sums + term
                mixed[1, o, b] += kern[b] * lift
                term = lift * back
                grad[b] = term if o == 0 else grad[b] + term
            mixed[0, o, a // 4] += jnp.where(mine, around(sums), 0.0)
        for b in range(packs):
            grads[:, pl.ds(pl.multiple_of((a * packs + b) * LANES, LANES), LANES)] = grad[b]
        return carry

    lax.fori_loop(0, ranks, blend, 0)

    def brow_copy(t, step):
        to = here.row_peer(step)
        return remote(back_row.at[t // tiles, to, lax.rem(t, tiles)], blocks.at[t, q, p],
                      brow_send.at[t, step], brow_recv.at[t, step], {"px": to})

    def bcross_copy(t):
        return remote(blocks.at[t, q], blocks.at[t, q], bcross_send.at[t], bcross_recv.at[t], here.cross)

    def bmate_copy(t, s):
        quarter = q if s == 0 else lax.rem(q + 2, py)
        return remote(blocks.at[t, quarter], blocks.at[t, quarter],
                      bmate_send.at[t, s], bmate_recv.at[t, s], here.mate)

    share = partial.shape[0] // px

    def rs_copy(step):
        to = here.row_peer(step)
        return remote(partial.at[pl.ds(to * share, share)], ranks_in.at[p], rs_send.at[step], rs_recv.at[step],
                      {"px": to})

    def cs_copy(step):
        to = here.col_peer(step)
        return remote(ranks_sum.at[to], ranks_col.at[q], cs_send.at[step], cs_recv.at[step], {"py": to})

    def ag_copy(step):
        return remote(core_all.at[p, q], core_all.at[p, q], ag_send.at[step], ag_recv.at[step],
                      {"px": here.row_peer(step)})

    def bg_copy(s):
        quarter = lax.rem(q + 2, py) if s == 2 else q
        return remote(core_all.at[:, quarter], core_all.at[:, quarter], bg_send.at[s], bg_recv.at[s],
                      here.cross if s == 0 else here.mate)

    def pr_copy(step):
        return remote(pack_sum.at[0], pack_row.at[p], pr_send.at[step], pr_recv.at[step],
                      {"px": here.row_peer(step)})

    def pc_copy(step):
        return remote(pack_sum.at[1], pack_col.at[q], pc_send.at[step], pc_recv.at[step],
                      {"py": here.col_peer(step)})

    def rows_out(f):
        pieces = [jnp.concatenate([mixed[f, o, b] for b in range(packs)], axis=1) for o in range(2)]
        lines = jnp.concatenate(pieces, axis=0)
        if f == 1:
            lines = lines * jnp.concatenate([scale] * packs, axis=1)
        back_row[f] = mul3((txb_ref[0], txb_ref[1]), halves(lines)).reshape(back_row.shape[1:])
        for t in range(f * tiles, (f + 1) * tiles):
            for step in range(1, px):
                brow_copy(t, step).start()
            blocks[t, q, p] = back_row[f, p, t - f * tiles]

    rows_out(0)
    whole = grads[...]
    thin = exact(first_ref[...], whole)
    tall = jnp.concatenate([thin[:, a * wide:(a + 1) * wide] for a in range(ranks)], axis=0)
    broad = widen()
    part = exact(tall, broad, NT)
    partial[...] = part
    for step in range(1, px):
        rs_copy(step).start()
    ranks_in[p] = partial[pl.ds(pl.multiple_of(p * share, share), share), :]
    rows_out(1)
    tables[1].wait()

    spread_rows = jnp.concatenate([kernel_rows[a * r1:(a + 1) * r1, :] for a in range(ranks)], axis=1)
    grad_first = exact(spread_rows, whole, NT)
    cross = exact(folded(), tall, TN)
    cross = jnp.where(one_hot(LANES, wide, lambda r: r % ranks, lambda c: c // m3), cross, 0.0)
    cross = cross.reshape(r3, ranks, wide).sum(axis=1)
    cross = exact(one_hot(r3, r3, lambda r: (r3 - r) % r3, lambda c: c).astype(F32), cross)
    grad_third = exact(cross, one_hot(wide, m3, lambda r: r % m3, lambda c: c).astype(F32))
    lane = iota((r1, LANES), 1)
    row = iota((r1, LANES), 0)
    small = exact(grad_first, one_hot(m1, LANES, lambda r: r, lambda c: c).astype(F32))
    small = small + exact(grad_third, one_hot(m3, LANES, lambda r: r + m1, lambda c: c).astype(F32))

    def second(a, sums):
        rows = partial[pl.ds(pl.multiple_of(a * r1, r1), r1), :]
        sums = list(sums)
        for r in range(r1):
            cell = unfold(rows[r:r + 1], r3, ranks)[:, :ranks]
            for s in range(r2):
                sums[s] = sums[s] + core[a, r, s] * cell
        return tuple(sums)

    sums = lax.fori_loop(0, ranks, second, tuple(jnp.zeros((r3, ranks), F32) for _ in range(r2)))
    for s in range(r2):
        small = small + jnp.where((lane == k + m1 + m3) & (row == s), jnp.sum(sums[s]), 0.0)
    pack_sum[0, ranks:ranks + r1] = small

    def slot(t):
        return jnp.maximum(t - tiles + 1, 0)

    def place(t):
        here_slot = slot(t)
        high, low = halves(blocks[t].reshape(-1, wide))
        modes = mul3((tyb[0], tyb[1]), (high, low))
        high, low = halves(modes)
        for x in range(group):
            for a in range(packs):
                for o in range(2):
                    part = (slice((x * 2 + o) * cols, (x * 2 + o + 1) * cols), slice(a * LANES, (a + 1) * LANES))
                    spot = (slice((x * packs + a) * cols, (x * packs + a + 1) * cols),
                            slice(o * LANES, (o + 1) * LANES))
                    back_h[spot] = high[part]
                    back_l[spot] = low[part]
        real = mul3((back_h[...], back_l[...]), (tzb_ref[0], tzb_ref[1]))
        high, low = halves(real)
        for x in range(group):
            for a in range(ranks):
                for h in range(cols // SUB):
                    row = (x * packs + a // 4) * cols + h * SUB
                    part = (slice(row, row + SUB), slice((a % 4) * depth, (a % 4 + 1) * depth))
                    spot = (here_slot, x, slice(a * SUB, (a + 1) * SUB), slice(h * depth, (h + 1) * depth))
                    real_h[spot] = high[part]
                    real_l[spot] = low[part]

    def outer(t):
        def one(x, carry):
            sides = [tile[t, :, x, h * SUB:(h + 1) * SUB, :].reshape(channels * SUB, depth)
                     for h in range(cols // SUB)]
            cells = jnp.concatenate(sides, axis=1)
            totals[t // tiles] += mul(cells, real_h[slot(t), x], NT) + mul(cells, real_l[slot(t), x], NT)
            return carry

        lax.fori_loop(0, group, one, 0)

    def real_copies(t):
        u = t - tiles
        return [pltpu.make_async_copy(real_h.at[u + 1], real_h_out.at[u], real_sem.at[u, 0]),
                pltpu.make_async_copy(real_l.at[u + 1], real_l_out.at[u], real_sem.at[u, 1])]

    def back_body(i, carry):
        @pl.when(i < steps)
        def _():
            for step in range(1, px):
                brow_copy(i, step).wait_recv()
            bcross_copy(i).start()
            bmate_copy(i, 0).start()

        @pl.when((i >= 2) & (i < steps + 2))
        def _():
            bcross_copy(i - 2).wait_recv()
            bmate_copy(i - 2, 1).start()

        @pl.when(i >= 3)
        def _():
            t = i - 3
            for s in range(2):
                bmate_copy(t, s).wait_recv()
            place(t)
            outer(t)

        @pl.when(i >= 3 + tiles)
        def _():
            for copy in real_copies(i - 3):
                copy.start()

        @pl.when(i == 5)
        def _():
            for step in range(1, px):
                rs_copy(step).wait_recv()
            for s in range(r2):
                total = None
                for o in range(px):
                    term = ranks_in[o] * second_ref[s, q * px + o]
                    total = term if total is None else total + term
                ranks_sum[s // 2, s % 2] = total
            ranks_col[q] = ranks_sum[q]
            for step in range(1, py):
                cs_copy(step).start()

        @pl.when(i == 6)
        def _():
            for step in range(1, py):
                cs_copy(step).wait_recv()
            total = ranks_col[0]
            for s in range(1, py):
                total = total + ranks_col[s]
            core_all[p, q] = total
            for step in range(1, px):
                ag_copy(step).start()

        @pl.when(i == 8)
        def _():
            for step in range(1, px):
                ag_copy(step).wait_recv()
            bg_copy(0).start()
            bg_copy(1).start()

        return carry

    lax.fori_loop(0, steps + 3, back_body, 0)
    bg_copy(0).wait_recv()
    bg_copy(2).start()
    keep = one_hot(channels * SUB, ranks * SUB, lambda r: r % SUB, lambda c: c % SUB)
    grids = [jnp.where(keep, totals[f], 0.0).reshape(channels, SUB, ranks * SUB).sum(axis=1) for f in range(2)]
    pick = one_hot(ranks, ranks * SUB, lambda r: r, lambda c: c // SUB).astype(F32)
    pack_sum[0, :ranks] = exact(pick, jnp.concatenate(grids, axis=0), NT)
    for step in range(1, px):
        pr_copy(step).start()
    pack_row[p] = pack_sum[0]
    bg_copy(1).wait_recv()
    bg_copy(2).wait_recv()
    core_out[...] = core_all[...]
    for step in range(1, px):
        pr_copy(step).wait_recv()
    total = pack_row[0]
    for s in range(1, px):
        total = total + pack_row[s]
    pack_sum[1] = total
    for step in range(1, py):
        pc_copy(step).start()
    pack_col[q] = total

    def drain(t, carry):
        for copy in mate_copies(t):
            copy.wait_send()
        cross_copy(t).wait_send()
        bcross_copy(t).wait_send()
        for s in range(2):
            bmate_copy(t, s).wait_send()
        for step in range(1, px):
            row_copy(t, step).wait_send()
            brow_copy(t, step).wait_send()
        return carry

    lax.fori_loop(0, steps, drain, 0)
    for step in range(1, px):
        for copy in (rs_copy, ag_copy, pr_copy):
            copy(step).wait_send()
    for s in range(3):
        bg_copy(s).wait_send()
    for t in range(tiles, steps):
        for copy in real_copies(t):
            copy.wait()
    for step in range(1, py):
        cs_copy(step).wait_send()
        pc_copy(step).wait_recv()
    total = pack_col[0]
    for s in range(1, py):
        total = total + pack_col[s]
    pack_out[...] = total
    for step in range(1, py):
        pc_copy(step).wait_send()


def emit_kernel(high_ref, low_ref, core_ref, pack_ref, wout_ref, out_ref, core_out, in_out, oo_out,
                first_out, second_out, third_out, kron):
    ranks, channels = wout_ref.shape
    cols, depth = out_ref.shape[2:]
    _, r1, r2, r3, _ = core_out.shape
    m1, m3 = first_out.shape[1], third_out.shape[1]
    m2 = second_out.shape[1]

    @pl.when(pl.program_id(0) == 0)
    def _():
        kron[0], kron[1] = spread(wout_ref[...], NT)
        in_out[...] = pack_ref[:ranks, :channels]
        oo_out[...] = pack_ref[:ranks, channels:2 * channels]
        first_out[...] = pack_ref[ranks:ranks + r1, :m1]
        third_out[...] = pack_ref[ranks:ranks + r1, m1:m1 + m3]
        second_out[...] = pack_ref[ranks:ranks + r1, m1 + m3:m1 + m3 + m2]

    def one(x, carry):
        both = mul3((kron[0], kron[1]), (high_ref[0, x], low_ref[0, x])).astype(BF16)
        for h in range(cols // SUB):
            out_ref[:, x, h * SUB:(h + 1) * SUB, :] = both[:, h * depth:(h + 1) * depth].reshape(
                channels, SUB, depth)
        return carry

    lax.fori_loop(0, out_ref.shape[1], one, 0)
    per = core_ref.shape[2]

    def two(a, carry):
        for s in range(r2):
            rows = core_ref[0, s // per, s % per, pl.ds(pl.multiple_of(a * r1, r1), r1), :]
            for r in range(r1):
                core_out[a, r, s] = unfold(rows[r:r + 1], r3, ranks)[:, :ranks]
        return carry

    lax.fori_loop(0, core_out.shape[0], two, 0)


def fast_shards(px, py, flow_field, cotangent, tucker_core, in_factor, out_factor,
                first_factor, second_factor, third_factor):
    channels, rows, cols, depth = flow_field.shape
    ri, ro, r1, r2, r3 = tucker_core.shape
    group = 2 * LANES // (2 * cols)
    tiles = rows // group
    steps = 2 * tiles
    packs = ri // 4
    wide = packs * LANES
    keep = px
    inverse_count = 1.0 / (NX * NY * NZ)

    small = np_depth(NZ, M3)
    tz = np.einsum("st,pzm->szptm", np.eye(4), small).reshape(4 * depth, 2 * 4 * M3)
    turn = np_turn(M2, NY).reshape(2, py, cols, 2, py, keep)
    ty = np.einsum("pdyoqk,xw->dqkxowpy", turn, np.eye(group))
    ty = ty.reshape(py, py * keep * group * 2, group * 2 * cols)
    turn = np_turn(M1, NX).reshape(2, NX, 2, M1)
    tx = turn.transpose(2, 3, 1, 0).reshape(2 * M1, NX * 2)
    tz_f, tz_b = np_halves(tz), np_halves(tz.T)
    ty_f = np_halves(ty).swapaxes(0, 1)
    ty_b = np_halves(ty.swapaxes(1, 2)).swapaxes(0, 1)
    tx_f, tx_b = np_halves(tx), np_halves(tx.T)
    weight = np.where(np.arange(M3) == 0, 1.0, 2.0) * inverse_count
    scale = jnp.asarray(np.tile(weight, 4)[None, :].astype(np.float32))

    vmem = pl.BlockSpec(memory_space=pltpu.VMEM)
    smem = pl.BlockSpec(memory_space=pltpu.SMEM)
    anywhere = pl.BlockSpec(memory_space=pl.ANY)
    shape = jax.ShapeDtypeStruct
    dma = pltpu.SemaphoreType.DMA

    def buf(*dims):
        return pltpu.VMEM(dims, F32)

    def thin(*dims):
        return pltpu.VMEM(dims, BF16)

    lines = group * packs * cols
    block = (keep, 2 * group, wide)
    real = (group, ri * SUB, cols // SUB * depth)
    count = ri * r1
    spectrum = (2, packs, M1, LANES)
    piece = (r2 // py, count // px, LANES)
    pack = (ri + r1, LANES)
    core = tucker_core.transpose(0, 2, 3, 4, 1)
    high, low, core_sum, packed = pl.pallas_call(
        functools.partial(remote_kernel, px, py),
        out_shape=(shape((tiles,) + real, BF16), shape((tiles,) + real, BF16),
                   shape((px, py) + piece, F32), shape(pack, F32)),
        in_specs=[smem] + [anywhere] * 5 + [vmem] * 9,
        out_specs=(anywhere, anywhere, vmem, vmem),
        scratch_shapes=[
            thin(steps, channels, group, cols, depth),
            thin(2, 2 * ri * SUB, channels * SUB),
            thin(lines, 4 * depth), thin(lines, 4 * depth),
            thin(group * 2 * cols, wide), thin(group * 2 * cols, wide),
            thin(*ty_f.shape[1:]), thin(*ty_b.shape[1:]), buf(*core.shape),
            buf(steps, py, *block), buf(steps, 2, *block), buf(steps, *block), buf(steps, *block),
            buf(steps, *block), buf(2, px, tiles, 2 * group, wide),
            buf(*spectrum), buf(*spectrum), buf(2, *spectrum),
            buf(count * r3, LANES), buf(count, wide), buf(M1, ri * wide),
            buf(2, px, tiles, 2 * group, wide), buf(steps, py, *block),
            thin(lines, 2 * LANES), thin(lines, 2 * LANES), thin(tiles + 1, *real), thin(tiles + 1, *real),
            buf(2, channels * SUB, ri * SUB),
            buf(count, LANES), buf(px, count // px, LANES), buf(py, *piece), buf(py, *piece),
            buf(px, py, *piece), buf(2, *pack), buf(px, *pack), buf(py, *pack),
            dma((steps,)), dma((3,)),
            dma((steps, 2)), dma((steps, 2)), dma((steps,)), dma((steps,)), dma((steps, px)), dma((steps, px)),
            dma((steps, px)), dma((steps, px)), dma((steps,)), dma((steps,)), dma((steps, 2)), dma((steps, 2)),
            dma((tiles, 2)),
            dma((px,)), dma((px,)), dma((py,)), dma((py,)), dma((px,)), dma((px,)), dma((3,)), dma((3,)),
            dma((px,)), dma((px,)), dma((py,)), dma((py,)),
        ],
        compiler_params=pltpu.CompilerParams(
            vmem_limit_bytes=VMEM_LIMIT, collective_id=0, has_side_effects=True),
    )(second_factor.T, flow_field, cotangent, jnp.asarray(ty_f), jnp.asarray(ty_b), core, in_factor.T,
      out_factor.T, first_factor.T, third_factor.T, scale,
      jnp.asarray(tz_f), jnp.asarray(tx_f), jnp.asarray(tz_b), jnp.asarray(tx_b))

    span = rows // px
    whole = lambda *dims: pl.BlockSpec(dims, lambda i: (0,) * len(dims))
    out, core_grad, in_grad, out_grad, first_grad, second_grad, third_grad = pl.pallas_call(
        emit_kernel, grid=(px,),
        out_shape=(
            shape(flow_field.shape, BF16), shape(core.shape, F32), shape((ri, channels), F32),
            shape((ro, channels), F32), shape((r1, M1), F32), shape((r2, M2), F32), shape((r3, M3), F32),
        ),
        in_specs=[
            pl.BlockSpec((1, span) + real[1:], lambda i: (i * span // group, i % (group // span), 0, 0)),
            pl.BlockSpec((1, span) + real[1:], lambda i: (i * span // group, i % (group // span), 0, 0)),
            pl.BlockSpec((1,) + (py,) + piece, lambda i: (i, 0, 0, 0, 0)),
            whole(*pack), whole(ro, channels),
        ],
        out_specs=(
            pl.BlockSpec((channels, span, cols, depth), lambda i: (0, i, 0, 0)),
            pl.BlockSpec((ri // px, r1, r2, r3, ro), lambda i: (i, 0, 0, 0, 0)),
            whole(ri, channels), whole(ro, channels), whole(r1, M1), whole(r2, M2), whole(r3, M3),
        ),
        scratch_shapes=[thin(2, channels * SUB, ro * SUB)],
        compiler_params=pltpu.CompilerParams(vmem_limit_bytes=VMEM_LIMIT),
    )(high, low, core_sum, packed, out_factor.T)
    return (out, core_grad.transpose(0, 4, 1, 2, 3), in_grad.T, out_grad.T, first_grad.T, second_grad.T,
            third_grad.T)


def solution(mesh):
    px, py = mesh.shape["px"], mesh.shape["py"]
    rows, cols = NX // px, NY // py
    fits = py == 4 and px * py == M2 and cols == 32 and rows == 16 and NZ == LANES
    fits = fits and M1 == 32 and M3 == 32
    body = functools.partial(fast_shards, px, py) if fits else shards
    return jax.shard_map(
        body,
        mesh=mesh,
        in_specs=(
            P(None, "px", "py", None),
            P(None, "px", "py", None),
            P(),
            P(),
            P(),
            P(),
            P(),
            P(),
        ),
        out_specs=(P(None, "px", "py", None), P(), P(), P(), P(), P(), P()),
        check_vma=False,
    )
```

```python
import functools
import math

import jax
import jax.numpy as jnp
import numpy as np
from jax import lax
from jax.experimental import pallas as pl
from jax.experimental.pallas import tpu as pltpu
from jax.sharding import PartitionSpec as P

NX = 128
NY = 128
NZ = 128
M1 = 32
M2 = 32
M3 = 32


HIGHEST = lax.Precision.HIGHEST


def turn_table(count, length):
    position = jnp.arange(count)
    frequency = jnp.where(position < count // 2, position, position - count)
    cells_at = jnp.arange(length)
    phase = frequency[None, :] * cells_at[:, None] % length
    angle = 2.0 * math.pi / length * phase.astype(jnp.float32)
    cosine = jnp.cos(angle)
    sine = jnp.sin(angle)
    upper = jnp.stack([cosine, -sine], axis=1)
    lower = jnp.stack([sine, cosine], axis=1)
    return jnp.stack([upper, lower])


def depth_table(length, count):
    cells_at = jnp.arange(length)
    frequency = jnp.arange(count)
    phase = cells_at[:, None] * frequency[None, :] % length
    angle = 2.0 * math.pi / length * phase.astype(jnp.float32)
    return jnp.concatenate([jnp.cos(angle), -jnp.sin(angle)], axis=1)


def to_modes(fields, depth_tables):
    across = turn_table(M2, NY)
    along = turn_table(M1, NX)
    spectra = []
    for member, z_table in zip(fields, depth_tables):
        channels, rows_here, cols_here, depth_len = member.shape
        flat = jnp.dot(member.reshape(-1, depth_len), z_table, precision=HIGHEST)
        spectra.append(flat.reshape(channels, rows_here, cols_here, 2, M3))
    members = lax.all_to_all(tuple(spectra), "py", split_axis=4, concat_axis=2, tiled=True)
    lines = tuple(
        (jnp.einsum("cxypm,pyqk->cxqkm", member, across, precision=HIGHEST) for member in members)
    )
    members = (
        lax.all_to_all(lines[0], "px", split_axis=3, concat_axis=1, tiled=True),
        lax.all_to_all(lines[1], "px", split_axis=3, concat_axis=1, tiled=True),
    )
    return tuple(
        (jnp.einsum("cxpkm,pxqj->cqjkm", member, along, precision=HIGHEST) for member in members)
    )


def to_space(modes, depth_weights):
    across = turn_table(M2, NY)
    along = turn_table(M1, NX)
    depth_base = depth_table(NZ, M3).T.reshape(2, M3, NZ)
    lines = tuple(
        (jnp.einsum("cqjkm,pxqj->cpxkm", member, along, precision=HIGHEST) for member in modes)
    )
    members = (
        lax.all_to_all(lines[0], "px", split_axis=2, concat_axis=3, tiled=True),
        lax.all_to_all(lines[1], "px", split_axis=2, concat_axis=3, tiled=True),
    )
    columns = tuple(
        (jnp.einsum("cqxkm,pyqk->cpxym", member, across, precision=HIGHEST) for member in members)
    )
    members = (
        lax.all_to_all(columns[0], "py", split_axis=3, concat_axis=4, tiled=True),
        lax.all_to_all(columns[1], "py", split_axis=3, concat_axis=4, tiled=True),
    )
    return tuple(
        (
            jnp.einsum(
                "cpxyk,pkn->cxyn", member, depth_base * weight_row[None, :, None], precision=HIGHEST
            )
            for member, weight_row in zip(members, depth_weights)
        )
    )


def shards(
    flow_field,
    cotangent,
    tucker_core,
    in_factor,
    out_factor,
    first_factor,
    second_factor,
    third_factor,
):
    inverse_count = 1.0 / (NX * NY * NZ)
    weights = jnp.where(jnp.arange(M3) == 0, 1.0, 2.0).astype(jnp.float32)
    unit_weights = jnp.ones((M3,), jnp.float32)
    base_table = depth_table(NZ, M3)
    weighted_table = base_table * jnp.concatenate([weights, weights])[None, :]
    block_second = M2 // lax.axis_size("px")
    block_third = M3 // lax.axis_size("py")
    start_second = lax.axis_index("px") * block_second
    start_third = lax.axis_index("py") * block_third

    def build_kernel(core_arg, first_arg, second_arg, third_arg):
        second_rows = lax.dynamic_slice_in_dim(second_arg, start_second, block_second, 0)
        third_rows = lax.dynamic_slice_in_dim(third_arg, start_third, block_third, 0)
        partial_core = jnp.einsum("abrst,mt->abrsm", core_arg, third_rows, precision=HIGHEST)
        partial_core = jnp.einsum("abrsm,ks->abrkm", partial_core, second_rows, precision=HIGHEST)
        return jnp.einsum("abrkm,jr->abjkm", partial_core, first_arg, precision=HIGHEST)

    kernel, pullback = jax.vjp(build_kernel, tucker_core, first_factor, second_factor, third_factor)
    field_wide = flow_field.astype(jnp.float32)
    back_wide = cotangent.astype(jnp.float32)
    lifted_grid = jnp.einsum("cxyn,ca->axyn", field_wide, in_factor, precision=HIGHEST)
    back_grid = jnp.einsum("cxyn,cb->bxyn", back_wide, out_factor, precision=HIGHEST)
    lifted, back_mixed = to_modes((lifted_grid, back_grid), (base_table, weighted_table))
    back_mixed = back_mixed * inverse_count
    mixed = jnp.einsum("abjkm,apjkm->bpjkm", kernel, lifted, precision=HIGHEST)
    grad_kernel = jnp.einsum("bpjkm,apjkm->abjkm", back_mixed, lifted, precision=HIGHEST)
    back_lifted = jnp.einsum("abjkm,bpjkm->apjkm", kernel, back_mixed, precision=HIGHEST)
    mixed_grid, lifted_back = to_space((mixed, back_lifted), (weights, unit_weights))
    mixed_grid = mixed_grid * inverse_count
    output_field = jnp.einsum("ob,bxyn->oxyn", out_factor, mixed_grid, precision=HIGHEST).astype(
        jnp.bfloat16
    )
    grad_out = jnp.einsum("oxyn,bxyn->ob", back_wide, mixed_grid, precision=HIGHEST)
    grad_in = jnp.einsum("ixyn,axyn->ia", field_wide, lifted_back, precision=HIGHEST)
    grad_core, grad_first, grad_second, grad_third = pullback(grad_kernel)
    totals = lax.psum(
        (grad_core, grad_in, grad_out, grad_first, grad_second, grad_third), ("px", "py")
    )
    return (output_field, totals[0], totals[1], totals[2], totals[3], totals[4], totals[5])


BF16 = jnp.bfloat16
F32 = jnp.float32
NN = (((1,), (0,)), ((), ()))
NT = (((1,), (1,)), ((), ()))
TN = (((0,), (0,)), ((), ()))
MESH = pl.DeviceIdType.MESH
VMEM_LIMIT = 63 * 1024 * 1024
SUB = 16
LANES = 128


def mul(a, b, dims=NN):
    return lax.dot_general(a, b, dims, preferred_element_type=F32)


def exact(a, b, dims=NN):
    return lax.dot_general(a, b, dims, precision=HIGHEST, preferred_element_type=F32)


def halves(x):
    high = x.astype(BF16)
    return high, (x - high.astype(F32)).astype(BF16)


def mul3(a, b, dims=NN):
    (ah, al), (bh, bl) = a, b
    return mul(ah, bh, dims) + (mul(ah, bl, dims) + mul(al, bh, dims))


def np_halves(x):
    x = np.asarray(x, np.float32)
    high = x.astype(BF16)
    return np.stack([high, (x - high.astype(np.float32)).astype(BF16)])


def np_turn(count, length):
    position = np.arange(count)
    frequency = np.where(position < count // 2, position, position - count)
    phase = frequency[None, :] * np.arange(length)[:, None] % length
    angle = 2.0 * np.pi / length * phase
    upper = np.stack([np.cos(angle), -np.sin(angle)], axis=1)
    lower = np.stack([np.sin(angle), np.cos(angle)], axis=1)
    return np.stack([upper, lower])


def np_depth(length, count):
    phase = np.arange(length)[:, None] * np.arange(count)[None, :] % length
    angle = 2.0 * np.pi / length * phase
    return np.stack([np.cos(angle), -np.sin(angle)])


def iota(shape, axis):
    return lax.broadcasted_iota(jnp.int32, shape, axis)


def one_hot(rows, cols, row_of, col_of):
    return row_of(iota((rows, cols), 0)) == col_of(iota((rows, cols), 1))


def spread(weights, dims):
    rows, cols = weights.shape if dims == NN else weights.shape[::-1]
    pick = one_hot(rows * SUB, rows, lambda r: r // SUB, lambda c: c).astype(F32).astype(BF16)
    lay = one_hot(cols * SUB, cols, lambda r: r // SUB, lambda c: c).astype(F32).astype(BF16)
    same = one_hot(rows * SUB, cols * SUB, lambda r: r % SUB, lambda c: c % SUB)
    result = []
    for part in halves(weights):
        tall = mul(pick, part, dims).astype(BF16)
        wide = mul(tall, lay, NT)
        result.append(jnp.where(same, wide, 0.0).astype(BF16))
    return result


def unfold(row, count, width):
    tall = jnp.broadcast_to(row, (count, row.shape[1]))
    return pltpu.roll(tall, 0, 1, stride=width, stride_axis=0)


class Place:
    def __init__(self, px, py):
        self.px, self.py = px, py
        self.p = lax.axis_index("px")
        self.q = lax.axis_index("py")
        self.core = lax.rem(self.q, 2)
        self.side = self.q // 2
        self.mate = {"py": self.q + 1 - 2 * self.core}
        self.cross = {"py": lax.rem(self.q + 2, py)}

    def row_peer(self, step):
        return lax.rem(self.p + step, self.px)

    def col_peer(self, step):
        return lax.rem(self.q + step, self.py)

    def greet(self):
        barrier = pltpu.get_barrier_semaphore()
        for step in range(1, self.px):
            pl.semaphore_signal(barrier, inc=1, device_id={"px": self.row_peer(step)}, device_id_type=MESH)
        for step in range(1, self.py):
            pl.semaphore_signal(barrier, inc=1, device_id={"py": self.col_peer(step)}, device_id_type=MESH)

    def meet(self):
        pl.semaphore_wait(pltpu.get_barrier_semaphore(), self.px + self.py - 2)


def remote(src, dst, send, recv, device):
    return pltpu.make_async_remote_copy(
        src_ref=src, dst_ref=dst, send_sem=send, recv_sem=recv, device_id=device, device_id_type=MESH,
    )


def remote_kernel(px, py, second_ref, flow_ref, cot_ref, tyf_ref, tyb_ref, core_ref, win_ref, wout_ref,
                  first_ref, third_ref, scale_ref, tzf_ref, txf_ref, tzb_ref, txb_ref,
                  out_ref, core_out, pack_out,
                  tile, kron, lines_h, lines_l, modes_h, modes_l, tyf, tyb, core, summed, from_mate, to_cross,
                  from_cross, to_row, gathered, lifted, backed, mixed, core_rows, kernel_rows, grads, back_row,
                  blocks, krono, real_h, real_l, totals, partial, ranks_in, ranks_sum, ranks_col,
                  core_all, pack_sum, pack_row, pack_col,
                  load_sem, table_sem, mate_send, mate_recv, cross_send, cross_recv, row_send, row_recv,
                  brow_send, brow_recv, bcross_send, bcross_recv, bmate_send, bmate_recv, out_sem,
                  rs_send, rs_recv, cs_send, cs_recv, ag_send, ag_recv, bg_send, bg_recv,
                  pr_send, pr_recv, pc_send, pc_recv):
    here = Place(px, py)
    p, q = here.p, here.q
    k = q * px + p
    steps, channels, group, cols, depth = tile.shape
    tiles = steps // 2
    ranks = win_ref.shape[0]
    packs = ranks // 4
    r1, m1 = first_ref.shape
    r3, m3 = third_ref.shape
    r2 = second_ref.shape[0]
    wide = packs * LANES

    here.greet()
    for t in range(steps):
        source = flow_ref if t < tiles else cot_ref
        pltpu.make_async_copy(
            source.at[:, pl.ds((t % tiles) * group, group)], tile.at[t], load_sem.at[t]).start()
    tables = [pltpu.make_async_copy(tyf_ref.at[q], tyf, table_sem.at[0]),
              pltpu.make_async_copy(tyb_ref.at[q], tyb, table_sem.at[1]),
              pltpu.make_async_copy(core_ref, core, table_sem.at[2])]
    for copy in tables[:2]:
        copy.start()
    for f, weight in enumerate((win_ref, wout_ref)):
        high, low = spread(weight[...], NN)
        kron[f, :ranks * SUB] = high
        kron[f, ranks * SUB:] = low
    totals[...] = jnp.zeros_like(totals)
    tables[0].wait()

    def mate_copies(t):
        return [remote(summed.at[t, 2 * s + 1 - here.core], from_mate.at[t, s],
                       mate_send.at[t, s], mate_recv.at[t, s], here.mate) for s in range(2)]

    def cross_copy(t):
        return remote(to_cross.at[t], from_cross.at[t], cross_send.at[t], cross_recv.at[t], here.cross)

    def row_copy(t, step):
        return remote(to_row.at[t, here.row_peer(step)], gathered.at[t // tiles, p, lax.rem(t, tiles)],
                      row_send.at[t, step], row_recv.at[t, step], {"px": here.row_peer(step)})

    def compute(t):
        f = t // tiles

        def lift(x, carry):
            sides = [tile[t, :, x, h * SUB:(h + 1) * SUB, :].reshape(channels * SUB, depth)
                     for h in range(cols // SUB)]
            both = mul(kron[f], jnp.concatenate(sides, axis=1))
            high, low = halves(both[:ranks * SUB] + both[ranks * SUB:])
            for a in range(ranks):
                for h in range(cols // SUB):
                    row = pl.multiple_of(x * (packs * cols) + (a // 4) * cols + h * SUB, SUB)
                    spot = (pl.ds(row, SUB), slice((a % 4) * depth, (a % 4 + 1) * depth))
                    part = (slice(a * SUB, (a + 1) * SUB), slice(h * depth, (h + 1) * depth))
                    lines_h[spot] = high[part]
                    lines_l[spot] = low[part]
            return carry

        lax.fori_loop(0, group, lift, 0)
        modes = mul3((lines_h[...], lines_l[...]), (tzf_ref[0], tzf_ref[1]))
        high, low = halves(modes)
        for x in range(group):
            for a in range(packs):
                for o in range(2):
                    spot = (slice((x * 2 + o) * cols, (x * 2 + o + 1) * cols), slice(a * LANES, (a + 1) * LANES))
                    part = (slice((x * packs + a) * cols, (x * packs + a + 1) * cols),
                            slice(o * LANES, (o + 1) * LANES))
                    modes_h[spot] = high[part]
                    modes_l[spot] = low[part]
        total = mul3((tyf[0], tyf[1]), (modes_h[...], modes_l[...]))
        summed[t] = total.reshape(summed.shape[1:])

    def kernel_side():
        tables[2].wait()

        def one(a, carry):
            for r in range(r1):
                total = second_ref[0, k] * core[a, r, 0]
                for s in range(1, r2):
                    total = total + second_ref[s, k] * core[a, r, s]
                core_rows[pl.ds(pl.multiple_of((a * r1 + r) * r3, r3), r3), :ranks] = total
            return carry

        core_rows[...] = jnp.zeros_like(core_rows)
        lax.fori_loop(0, ranks, one, 0)
        kernel_rows[...] = exact(folded(), widen())

    def folded():
        total = core_rows[pl.ds(0, ranks * r1, stride=r3), :]
        for t in range(1, r3):
            total = total + pltpu.roll(core_rows[pl.ds(t, ranks * r1, stride=r3), :], (r3 - t) * ranks, 1)
        return total

    def widen():
        tall = one_hot(LANES, r3, lambda r: (r3 - r // ranks) % r3, lambda c: c).astype(F32)
        flat = one_hot(m3, wide, lambda r: r, lambda c: c % m3).astype(F32)
        full = exact(exact(tall, third_ref[...]), flat)
        return jnp.where(one_hot(LANES, wide, lambda r: r % ranks, lambda c: c // m3), full, 0.0)

    def body(t, carry):
        @pl.when(t < steps)
        def _():
            pltpu.make_async_copy(flow_ref.at[:, pl.ds(0, group)], tile.at[t], load_sem.at[t]).wait()
            compute(t)

        @pl.when(t == 0)
        def _():
            here.meet()
            tables[2].start()

        @pl.when(t < steps)
        def _():
            for copy in mate_copies(t):
                copy.start()

        @pl.when((t >= 1) & (t < steps + 1))
        def _():
            u = t - 1
            for copy in mate_copies(u):
                copy.wait_recv()
            to_cross[u] = summed[u, 2 * (1 - here.side) + here.core] + from_mate[u, 1 - here.side]
            cross_copy(u).start()

        @pl.when(t == steps)
        def _():
            kernel_side()

        @pl.when(t >= 3)
        def _():
            u = t - 3
            cross_copy(u).wait_recv()
            to_row[u] = summed[u, 2 * here.side + here.core] + from_mate[u, here.side] + from_cross[u]
            for step in range(1, px):
                row_copy(u, step).start()
            gathered[u // tiles, p, lax.rem(u, tiles)] = to_row[u, p]

        return carry

    lax.fori_loop(0, steps + 3, body, 0)
    scale = scale_ref[...]

    def arrive(f):
        for t in range(f * tiles, (f + 1) * tiles):
            for step in range(1, px):
                row_copy(t, step).wait_recv()
        lines = mul3((txf_ref[0], txf_ref[1]), halves(gathered[f].reshape(-1, wide)))
        for o in range(2):
            for a in range(packs):
                cell = lines[o * m1:(o + 1) * m1, a * LANES:(a + 1) * LANES]
                if f == 0:
                    lifted[o, a] = cell
                else:
                    backed[o, a] = cell * scale

    group_of = iota((m1, LANES), 1) // m3
    lay = one_hot(r1 * LANES, r1, lambda r: r // LANES, lambda c: c).astype(F32)
    columns = exact(first_ref[...], lay, (((0,), (1,)), ((), ())))
    mixed[...] = jnp.zeros_like(mixed)

    def around(v):
        v = v + pltpu.roll(v, 64, 1)
        return v + pltpu.roll(v, 32, 1)

    def spots(a):
        return [pl.ds(pl.multiple_of((a * packs + b) * LANES, LANES), LANES) for b in range(packs)]

    def blend(a, carry):
        mine = group_of == lax.rem(a, 4)
        block = kernel_rows[pl.ds(pl.multiple_of(a * r1, r1), r1), :]
        lift = [around(jnp.where(mine, lifted[o, a // 4], 0.0)) for o in range(2)]
        for b, lanes in enumerate(spots(a)):
            total = columns[:, :LANES] * block[0:1, b * LANES:(b + 1) * LANES]
            for r in range(1, r1):
                total = total + columns[:, r * LANES:(r + 1) * LANES] * block[r:r + 1, b * LANES:(b + 1) * LANES]
            grads[:, lanes] = total
            for o in range(2):
                mixed[0, o, b] += total * lift[o]
        return carry

    def unblend(a, carry):
        mine = group_of == lax.rem(a, 4)
        lift = [around(jnp.where(mine, lifted[o, a // 4], 0.0)) for o in range(2)]
        sums = [None, None]
        for b, lanes in enumerate(spots(a)):
            total = grads[:, lanes]
            grad = None
            for o in range(2):
                back = backed[o, b]
                term = total * back
                sums[o] = term if sums[o] is None else sums[o] + term
                term = lift[o] * back
                grad = term if grad is None else grad + term
            grads[:, lanes] = grad
        for o in range(2):
            mixed[1, o, a // 4] += jnp.where(mine, around(sums[o]), 0.0)
        return carry

    def brow_copy(t, step):
        to = here.row_peer(step)
        return remote(back_row.at[t // tiles, to, lax.rem(t, tiles)], blocks.at[t, q, p],
                      brow_send.at[t, step], brow_recv.at[t, step], {"px": to})

    def bcross_copy(t):
        return remote(blocks.at[t, q], blocks.at[t, q], bcross_send.at[t], bcross_recv.at[t], here.cross)

    def bmate_copy(t, s):
        quarter = q if s == 0 else lax.rem(q + 2, py)
        return remote(blocks.at[t, quarter], blocks.at[t, quarter],
                      bmate_send.at[t, s], bmate_recv.at[t, s], here.mate)

    share = partial.shape[0] // px

    def rs_copy(step):
        to = here.row_peer(step)
        return remote(partial.at[pl.ds(to * share, share)], ranks_in.at[p], rs_send.at[step], rs_recv.at[step],
                      {"px": to})

    def cs_copy(step):
        to = here.col_peer(step)
        return remote(ranks_sum.at[to], ranks_col.at[q], cs_send.at[step], cs_recv.at[step], {"py": to})

    def ag_copy(step):
        return remote(core_all.at[p, q], core_all.at[p, q], ag_send.at[step], ag_recv.at[step],
                      {"px": here.row_peer(step)})

    def bg_copy(s):
        quarter = lax.rem(q + 2, py) if s == 2 else q
        return remote(core_all.at[:, quarter], core_all.at[:, quarter], bg_send.at[s], bg_recv.at[s],
                      here.cross if s == 0 else here.mate)

    def pr_copy(step):
        return remote(pack_sum.at[0], pack_row.at[p], pr_send.at[step], pr_recv.at[step],
                      {"px": here.row_peer(step)})

    def pc_copy(step):
        return remote(pack_sum.at[1], pack_col.at[q], pc_send.at[step], pc_recv.at[step],
                      {"py": here.col_peer(step)})

    def rows_out(f):
        pieces = [jnp.concatenate([mixed[f, o, b] for b in range(packs)], axis=1) for o in range(2)]
        lines = jnp.concatenate(pieces, axis=0)
        if f == 0:
            lines = lines * jnp.concatenate([scale] * packs, axis=1)
        back_row[f] = mul3((txb_ref[0], txb_ref[1]), halves(lines)).reshape(back_row.shape[1:])
        for t in range(f * tiles, (f + 1) * tiles):
            for step in range(1, px):
                brow_copy(t, step).start()
            blocks[t, q, p] = back_row[f, p, t - f * tiles]

    arrive(0)
    lax.fori_loop(0, ranks, blend, 0)
    rows_out(0)
    arrive(1)
    lax.fori_loop(0, ranks, unblend, 0)
    rows_out(1)
    tables[1].wait()
    high, low = spread(wout_ref[...], NT)
    krono[0] = high
    krono[1] = low

    def tall_grads():
        thin = exact(first_ref[...], grads[...])
        return jnp.concatenate([thin[:, a * wide:(a + 1) * wide] for a in range(ranks)], axis=0)

    def core_side():
        partial[...] = exact(tall_grads(), widen(), NT)
        for step in range(1, px):
            rs_copy(step).start()
        ranks_in[p] = partial[pl.ds(pl.multiple_of(p * share, share), share), :]

    def small_side():
        spread_rows = jnp.concatenate([kernel_rows[a * r1:(a + 1) * r1, :] for a in range(ranks)], axis=1)
        grad_first = exact(spread_rows, grads[...], NT)
        cross = exact(folded(), tall_grads(), TN)
        cross = jnp.where(one_hot(LANES, wide, lambda r: r % ranks, lambda c: c // m3), cross, 0.0)
        cross = cross.reshape(r3, ranks, wide).sum(axis=1)
        cross = exact(one_hot(r3, r3, lambda r: (r3 - r) % r3, lambda c: c).astype(F32), cross)
        grad_third = exact(cross, one_hot(wide, m3, lambda r: r % m3, lambda c: c).astype(F32))
        lane = iota((r1, LANES), 1)
        row = iota((r1, LANES), 0)
        small = exact(grad_first, one_hot(m1, LANES, lambda r: r, lambda c: c).astype(F32))
        small = small + exact(grad_third, one_hot(m3, LANES, lambda r: r + m1, lambda c: c).astype(F32))

        def second(a, sums):
            rows = partial[pl.ds(pl.multiple_of(a * r1, r1), r1), :]
            sums = list(sums)
            for r in range(r1):
                cell = unfold(rows[r:r + 1], r3, ranks)[:, :ranks]
                for s in range(r2):
                    sums[s] = sums[s] + core[a, r, s] * cell
            return tuple(sums)

        sums = lax.fori_loop(0, ranks, second, tuple(jnp.zeros((r3, ranks), F32) for _ in range(r2)))
        for s in range(r2):
            small = small + jnp.where((lane == k + m1 + m3) & (row == s), jnp.sum(sums[s]), 0.0)
        pack_sum[0, ranks:ranks + r1] = small

    def slot(t):
        return (t + 1) * (1 - t // tiles)

    def place(t):
        here_slot = slot(t)
        high, low = halves(blocks[t].reshape(-1, wide))
        modes = mul3((tyb[0], tyb[1]), (high, low))
        high, low = halves(modes)
        for x in range(group):
            for a in range(packs):
                for o in range(2):
                    part = (slice((x * 2 + o) * cols, (x * 2 + o + 1) * cols), slice(a * LANES, (a + 1) * LANES))
                    spot = (slice((x * packs + a) * cols, (x * packs + a + 1) * cols),
                            slice(o * LANES, (o + 1) * LANES))
                    lines_h[spot] = high[part]
                    lines_l[spot] = low[part]
        half = 2 * LANES
        real = mul3((lines_h[:, :half], lines_l[:, :half]), (tzb_ref[0], tzb_ref[1]))
        high, low = halves(real)
        for x in range(group):
            for a in range(ranks):
                for h in range(cols // SUB):
                    row = (x * packs + a // 4) * cols + h * SUB
                    part = (slice(row, row + SUB), slice((a % 4) * depth, (a % 4 + 1) * depth))
                    spot = (here_slot, x, slice(a * SUB, (a + 1) * SUB), slice(h * depth, (h + 1) * depth))
                    real_h[spot] = high[part]
                    real_l[spot] = low[part]

    def outer(t):
        u = lax.rem(t + tiles, steps)

        def one(x, carry):
            sides = [tile[u, :, x, h * SUB:(h + 1) * SUB, :].reshape(channels * SUB, depth)
                     for h in range(cols // SUB)]
            cells = jnp.concatenate(sides, axis=1)
            totals[u // tiles] += mul(cells, real_h[slot(t), x], NT) + mul(cells, real_l[slot(t), x], NT)
            return carry

        lax.fori_loop(0, group, one, 0)

    def out_copy(g):
        return pltpu.make_async_copy(tile.at[tiles + g], out_ref.at[:, pl.ds(g * group, group)], out_sem.at[g])

    def emit(g):
        def one(x, carry):
            both = mul3((krono[0], krono[1]), (real_h[g + 1, x], real_l[g + 1, x])).astype(BF16)
            for h in range(cols // SUB):
                tile[tiles + g, :, x, h * SUB:(h + 1) * SUB, :] = both[:, h * depth:(h + 1) * depth].reshape(
                    channels, SUB, depth)
            return carry

        lax.fori_loop(0, group, one, 0)
        out_copy(g).start()

    def back_body(i, carry):
        @pl.when(i < steps)
        def _():
            for step in range(1, px):
                brow_copy(i, step).wait_recv()
            bcross_copy(i).start()
            bmate_copy(i, 0).start()

        @pl.when((i >= 2) & (i < steps + 2))
        def _():
            bcross_copy(i - 2).wait_recv()
            bmate_copy(i - 2, 1).start()

        @pl.when(i >= 3)
        def _():
            t = i - 3
            for s in range(2):
                bmate_copy(t, s).wait_recv()
            place(t)
            outer(t)

        @pl.when((i >= tiles + 1) & (i < tiles + 3))
        def _():
            emit(i - tiles - 1)

        @pl.when(i == 2)
        def _():
            core_side()

        @pl.when(i == 3)
        def _():
            small_side()

        @pl.when(i == 5)
        def _():
            for step in range(1, px):
                rs_copy(step).wait_recv()
            for s in range(r2):
                total = None
                for o in range(px):
                    term = ranks_in[o] * second_ref[s, q * px + o]
                    total = term if total is None else total + term
                ranks_sum[s // 2, s % 2] = total
            ranks_col[q] = ranks_sum[q]
            for step in range(1, py):
                cs_copy(step).start()

        @pl.when(i == 7)
        def _():
            for step in range(1, py):
                cs_copy(step).wait_recv()
            total = ranks_col[0]
            for s in range(1, py):
                total = total + ranks_col[s]
            core_all[p, q] = total
            for step in range(1, px):
                ag_copy(step).start()

        @pl.when(i == 9)
        def _():
            for step in range(1, px):
                ag_copy(step).wait_recv()
            bg_copy(0).start()
            bg_copy(1).start()

        return carry

    lax.fori_loop(0, steps + 3, back_body, 0)
    bg_copy(0).wait_recv()
    bg_copy(2).start()
    keep = one_hot(channels * SUB, ranks * SUB, lambda r: r % SUB, lambda c: c % SUB)
    grids = [jnp.where(keep, totals[f], 0.0).reshape(channels, SUB, ranks * SUB).sum(axis=1) for f in range(2)]
    pick = one_hot(ranks, ranks * SUB, lambda r: r, lambda c: c // SUB).astype(F32)
    pack_sum[0, :ranks] = exact(pick, jnp.concatenate(grids, axis=0), NT)
    for step in range(1, px):
        pr_copy(step).start()
    pack_row[p] = pack_sum[0]
    emit(tiles - 2)
    bg_copy(1).wait_recv()
    bg_copy(2).wait_recv()
    core_out[...] = core_all[...]
    for step in range(1, px):
        pr_copy(step).wait_recv()
    total = pack_row[0]
    for s in range(1, px):
        total = total + pack_row[s]
    pack_sum[1] = total
    for step in range(1, py):
        pc_copy(step).start()
    pack_col[q] = total
    emit(tiles - 1)

    def drain(t, carry):
        for copy in mate_copies(t):
            copy.wait_send()
        cross_copy(t).wait_send()
        bcross_copy(t).wait_send()
        for s in range(2):
            bmate_copy(t, s).wait_send()
        for step in range(1, px):
            row_copy(t, step).wait_send()
            brow_copy(t, step).wait_send()
        return carry

    lax.fori_loop(0, steps, drain, 0)
    for step in range(1, px):
        for copy in (rs_copy, ag_copy, pr_copy):
            copy(step).wait_send()
    for s in range(3):
        bg_copy(s).wait_send()
    for step in range(1, py):
        cs_copy(step).wait_send()
        pc_copy(step).wait_recv()
    total = pack_col[0]
    for s in range(1, py):
        total = total + pack_col[s]
    pack_out[...] = total
    for step in range(1, py):
        pc_copy(step).wait_send()
    for g in range(tiles):
        out_copy(g).wait()


def emit_kernel(field_ref, core_ref, pack_ref, out_ref, core_out, in_out, oo_out,
                first_out, second_out, third_out):
    ranks, channels = in_out.shape
    _, r1, r2, r3, _ = core_out.shape
    m1, m3 = first_out.shape[1], third_out.shape[1]
    m2 = second_out.shape[1]

    @pl.when(pl.program_id(0) == 0)
    def _():
        in_out[...] = pack_ref[:ranks, :channels]
        oo_out[...] = pack_ref[:ranks, channels:2 * channels]
        first_out[...] = pack_ref[ranks:ranks + r1, :m1]
        third_out[...] = pack_ref[ranks:ranks + r1, m1:m1 + m3]
        second_out[...] = pack_ref[ranks:ranks + r1, m1 + m3:m1 + m3 + m2]

    out_ref[...] = field_ref[...]
    per = core_ref.shape[2]

    def two(a, carry):
        for s in range(r2):
            rows = core_ref[0, s // per, s % per, pl.ds(pl.multiple_of(a * r1, r1), r1), :]
            for r in range(r1):
                core_out[a, r, s] = unfold(rows[r:r + 1], r3, ranks)[:, :ranks]
        return carry

    lax.fori_loop(0, core_out.shape[0], two, 0)


def fast_shards(px, py, flow_field, cotangent, tucker_core, in_factor, out_factor,
                first_factor, second_factor, third_factor):
    channels, rows, cols, depth = flow_field.shape
    ri, ro, r1, r2, r3 = tucker_core.shape
    group = 2 * LANES // (2 * cols)
    tiles = rows // group
    steps = 2 * tiles
    packs = ri // 4
    wide = packs * LANES
    keep = px
    inverse_count = 1.0 / (NX * NY * NZ)

    small = np_depth(NZ, M3)
    tz = np.einsum("st,pzm->szptm", np.eye(4), small).reshape(4 * depth, 2 * 4 * M3)
    turn = np_turn(M2, NY).reshape(2, py, cols, 2, py, keep)
    ty = np.einsum("pdyoqk,xw->dqkxowpy", turn, np.eye(group))
    ty = ty.reshape(py, py * keep * group * 2, group * 2 * cols)
    turn = np_turn(M1, NX).reshape(2, NX, 2, M1)
    tx = turn.transpose(2, 3, 1, 0).reshape(2 * M1, NX * 2)
    tz_f, tz_b = np_halves(tz), np_halves(tz.T)
    ty_f = np_halves(ty).swapaxes(0, 1)
    ty_b = np_halves(ty.swapaxes(1, 2)).swapaxes(0, 1)
    tx_f, tx_b = np_halves(tx), np_halves(tx.T)
    weight = np.where(np.arange(M3) == 0, 1.0, 2.0) * inverse_count
    scale = jnp.asarray(np.tile(weight, 4)[None, :].astype(np.float32))

    vmem = pl.BlockSpec(memory_space=pltpu.VMEM)
    smem = pl.BlockSpec(memory_space=pltpu.SMEM)
    anywhere = pl.BlockSpec(memory_space=pl.ANY)
    shape = jax.ShapeDtypeStruct
    dma = pltpu.SemaphoreType.DMA

    def buf(*dims):
        return pltpu.VMEM(dims, F32)

    def thin(*dims):
        return pltpu.VMEM(dims, BF16)

    lines = group * packs * cols
    block = (keep, 2 * group, wide)
    real = (group, ri * SUB, cols // SUB * depth)
    count = ri * r1
    spectrum = (2, packs, M1, LANES)
    piece = (r2 // py, count // px, LANES)
    pack = (ri + r1, LANES)
    core = tucker_core.transpose(0, 2, 3, 4, 1)
    field, core_sum, packed = pl.pallas_call(
        functools.partial(remote_kernel, px, py),
        out_shape=(shape(flow_field.shape, BF16), shape((px, py) + piece, F32), shape(pack, F32)),
        in_specs=[smem] + [anywhere] * 5 + [vmem] * 9,
        out_specs=(anywhere, vmem, vmem),
        scratch_shapes=[
            thin(steps, channels, group, cols, depth),
            thin(2, 2 * ri * SUB, channels * SUB),
            thin(lines, 4 * depth), thin(lines, 4 * depth),
            thin(group * 2 * cols, wide), thin(group * 2 * cols, wide),
            thin(*ty_f.shape[1:]), thin(*ty_b.shape[1:]), buf(*core.shape),
            buf(steps, py, *block), buf(steps, 2, *block), buf(steps, *block), buf(steps, *block),
            buf(steps, *block), buf(2, px, tiles, 2 * group, wide),
            buf(*spectrum), buf(*spectrum), buf(2, *spectrum),
            buf(count * r3, LANES), buf(count, wide), buf(M1, ri * wide),
            buf(2, px, tiles, 2 * group, wide), buf(steps, py, *block),
            thin(2, channels * SUB, ro * SUB), thin(tiles + 1, *real), thin(tiles + 1, *real),
            buf(2, channels * SUB, ri * SUB),
            buf(count, LANES), buf(px, count // px, LANES), buf(py, *piece), buf(py, *piece),
            buf(px, py, *piece), buf(2, *pack), buf(px, *pack), buf(py, *pack),
            dma((steps,)), dma((3,)),
            dma((steps, 2)), dma((steps, 2)), dma((steps,)), dma((steps,)), dma((steps, px)), dma((steps, px)),
            dma((steps, px)), dma((steps, px)), dma((steps,)), dma((steps,)), dma((steps, 2)), dma((steps, 2)),
            dma((tiles,)),
            dma((px,)), dma((px,)), dma((py,)), dma((py,)), dma((px,)), dma((px,)), dma((3,)), dma((3,)),
            dma((px,)), dma((px,)), dma((py,)), dma((py,)),
        ],
        compiler_params=pltpu.CompilerParams(
            vmem_limit_bytes=VMEM_LIMIT, collective_id=0, has_side_effects=True),
    )(second_factor.T, flow_field, cotangent, jnp.asarray(ty_f), jnp.asarray(ty_b), core, in_factor.T,
      out_factor.T, first_factor.T, third_factor.T, scale,
      jnp.asarray(tz_f), jnp.asarray(tx_f), jnp.asarray(tz_b), jnp.asarray(tx_b))

    span = rows // px
    whole = lambda *dims: pl.BlockSpec(dims, lambda i: (0,) * len(dims))
    out, core_grad, in_grad, out_grad, first_grad, second_grad, third_grad = pl.pallas_call(
        emit_kernel, grid=(px,),
        out_shape=(
            shape(flow_field.shape, BF16), shape(core.shape, F32), shape((ri, channels), F32),
            shape((ro, channels), F32), shape((r1, M1), F32), shape((r2, M2), F32), shape((r3, M3), F32),
        ),
        in_specs=[
            pl.BlockSpec((channels, span, cols, depth), lambda i: (0, i, 0, 0)),
            pl.BlockSpec((1,) + (py,) + piece, lambda i: (i, 0, 0, 0, 0)),
            whole(*pack),
        ],
        out_specs=(
            pl.BlockSpec((channels, span, cols, depth), lambda i: (0, i, 0, 0)),
            pl.BlockSpec((ri // px, r1, r2, r3, ro), lambda i: (i, 0, 0, 0, 0)),
            whole(ri, channels), whole(ro, channels), whole(r1, M1), whole(r2, M2), whole(r3, M3),
        ),
        compiler_params=pltpu.CompilerParams(vmem_limit_bytes=VMEM_LIMIT),
    )(field, core_sum, packed)
    return (out, core_grad.transpose(0, 4, 1, 2, 3), in_grad.T, out_grad.T, first_grad.T, second_grad.T,
            third_grad.T)


def solution(mesh):
    px, py = mesh.shape["px"], mesh.shape["py"]
    rows, cols = NX // px, NY // py
    fits = py == 4 and px * py == M2 and cols == 32 and rows == 16 and NZ == LANES
    fits = fits and M1 == 32 and M3 == 32
    body = functools.partial(fast_shards, px, py) if fits else shards
    return jax.shard_map(
        body,
        mesh=mesh,
        in_specs=(
            P(None, "px", "py", None),
            P(None, "px", "py", None),
            P(),
            P(),
            P(),
            P(),
            P(),
            P(),
        ),
        out_specs=(P(None, "px", "py", None), P(), P(), P(), P(), P(), P()),
        check_vma=False,
    )
```

```python
import functools
import math

import jax
import jax.numpy as jnp
import numpy as np
from jax import lax
from jax.experimental import pallas as pl
from jax.experimental.pallas import tpu as pltpu
from jax.sharding import PartitionSpec as P

NX = 128
NY = 128
NZ = 128
M1 = 32
M2 = 32
M3 = 32


HIGHEST = lax.Precision.HIGHEST


def turn_table(count, length):
    position = jnp.arange(count)
    frequency = jnp.where(position < count // 2, position, position - count)
    cells_at = jnp.arange(length)
    phase = frequency[None, :] * cells_at[:, None] % length
    angle = 2.0 * math.pi / length * phase.astype(jnp.float32)
    cosine = jnp.cos(angle)
    sine = jnp.sin(angle)
    upper = jnp.stack([cosine, -sine], axis=1)
    lower = jnp.stack([sine, cosine], axis=1)
    return jnp.stack([upper, lower])


def depth_table(length, count):
    cells_at = jnp.arange(length)
    frequency = jnp.arange(count)
    phase = cells_at[:, None] * frequency[None, :] % length
    angle = 2.0 * math.pi / length * phase.astype(jnp.float32)
    return jnp.concatenate([jnp.cos(angle), -jnp.sin(angle)], axis=1)


def to_modes(fields, depth_tables):
    across = turn_table(M2, NY)
    along = turn_table(M1, NX)
    spectra = []
    for member, z_table in zip(fields, depth_tables):
        channels, rows_here, cols_here, depth_len = member.shape
        flat = jnp.dot(member.reshape(-1, depth_len), z_table, precision=HIGHEST)
        spectra.append(flat.reshape(channels, rows_here, cols_here, 2, M3))
    members = lax.all_to_all(tuple(spectra), "py", split_axis=4, concat_axis=2, tiled=True)
    lines = tuple(
        (jnp.einsum("cxypm,pyqk->cxqkm", member, across, precision=HIGHEST) for member in members)
    )
    members = (
        lax.all_to_all(lines[0], "px", split_axis=3, concat_axis=1, tiled=True),
        lax.all_to_all(lines[1], "px", split_axis=3, concat_axis=1, tiled=True),
    )
    return tuple(
        (jnp.einsum("cxpkm,pxqj->cqjkm", member, along, precision=HIGHEST) for member in members)
    )


def to_space(modes, depth_weights):
    across = turn_table(M2, NY)
    along = turn_table(M1, NX)
    depth_base = depth_table(NZ, M3).T.reshape(2, M3, NZ)
    lines = tuple(
        (jnp.einsum("cqjkm,pxqj->cpxkm", member, along, precision=HIGHEST) for member in modes)
    )
    members = (
        lax.all_to_all(lines[0], "px", split_axis=2, concat_axis=3, tiled=True),
        lax.all_to_all(lines[1], "px", split_axis=2, concat_axis=3, tiled=True),
    )
    columns = tuple(
        (jnp.einsum("cqxkm,pyqk->cpxym", member, across, precision=HIGHEST) for member in members)
    )
    members = (
        lax.all_to_all(columns[0], "py", split_axis=3, concat_axis=4, tiled=True),
        lax.all_to_all(columns[1], "py", split_axis=3, concat_axis=4, tiled=True),
    )
    return tuple(
        (
            jnp.einsum(
                "cpxyk,pkn->cxyn", member, depth_base * weight_row[None, :, None], precision=HIGHEST
            )
            for member, weight_row in zip(members, depth_weights)
        )
    )


def shards(
    flow_field,
    cotangent,
    tucker_core,
    in_factor,
    out_factor,
    first_factor,
    second_factor,
    third_factor,
):
    inverse_count = 1.0 / (NX * NY * NZ)
    weights = jnp.where(jnp.arange(M3) == 0, 1.0, 2.0).astype(jnp.float32)
    unit_weights = jnp.ones((M3,), jnp.float32)
    base_table = depth_table(NZ, M3)
    weighted_table = base_table * jnp.concatenate([weights, weights])[None, :]
    block_second = M2 // lax.axis_size("px")
    block_third = M3 // lax.axis_size("py")
    start_second = lax.axis_index("px") * block_second
    start_third = lax.axis_index("py") * block_third

    def build_kernel(core_arg, first_arg, second_arg, third_arg):
        second_rows = lax.dynamic_slice_in_dim(second_arg, start_second, block_second, 0)
        third_rows = lax.dynamic_slice_in_dim(third_arg, start_third, block_third, 0)
        partial_core = jnp.einsum("abrst,mt->abrsm", core_arg, third_rows, precision=HIGHEST)
        partial_core = jnp.einsum("abrsm,ks->abrkm", partial_core, second_rows, precision=HIGHEST)
        return jnp.einsum("abrkm,jr->abjkm", partial_core, first_arg, precision=HIGHEST)

    kernel, pullback = jax.vjp(build_kernel, tucker_core, first_factor, second_factor, third_factor)
    field_wide = flow_field.astype(jnp.float32)
    back_wide = cotangent.astype(jnp.float32)
    lifted_grid = jnp.einsum("cxyn,ca->axyn", field_wide, in_factor, precision=HIGHEST)
    back_grid = jnp.einsum("cxyn,cb->bxyn", back_wide, out_factor, precision=HIGHEST)
    lifted, back_mixed = to_modes((lifted_grid, back_grid), (base_table, weighted_table))
    back_mixed = back_mixed * inverse_count
    mixed = jnp.einsum("abjkm,apjkm->bpjkm", kernel, lifted, precision=HIGHEST)
    grad_kernel = jnp.einsum("bpjkm,apjkm->abjkm", back_mixed, lifted, precision=HIGHEST)
    back_lifted = jnp.einsum("abjkm,bpjkm->apjkm", kernel, back_mixed, precision=HIGHEST)
    mixed_grid, lifted_back = to_space((mixed, back_lifted), (weights, unit_weights))
    mixed_grid = mixed_grid * inverse_count
    output_field = jnp.einsum("ob,bxyn->oxyn", out_factor, mixed_grid, precision=HIGHEST).astype(
        jnp.bfloat16
    )
    grad_out = jnp.einsum("oxyn,bxyn->ob", back_wide, mixed_grid, precision=HIGHEST)
    grad_in = jnp.einsum("ixyn,axyn->ia", field_wide, lifted_back, precision=HIGHEST)
    grad_core, grad_first, grad_second, grad_third = pullback(grad_kernel)
    totals = lax.psum(
        (grad_core, grad_in, grad_out, grad_first, grad_second, grad_third), ("px", "py")
    )
    return (output_field, totals[0], totals[1], totals[2], totals[3], totals[4], totals[5])


BF16 = jnp.bfloat16
F32 = jnp.float32
NN = (((1,), (0,)), ((), ()))
NT = (((1,), (1,)), ((), ()))
TN = (((0,), (0,)), ((), ()))
MESH = pl.DeviceIdType.MESH
VMEM_LIMIT = 63 * 1024 * 1024
SUB = 16
LANES = 128


def mul(a, b, dims=NN):
    return lax.dot_general(a, b, dims, preferred_element_type=F32)


def exact(a, b, dims=NN):
    return lax.dot_general(a, b, dims, precision=HIGHEST, preferred_element_type=F32)


def halves(x):
    high = x.astype(BF16)
    return high, (x - high.astype(F32)).astype(BF16)


def mul3(a, b, dims=NN):
    (ah, al), (bh, bl) = a, b
    return mul(ah, bh, dims) + (mul(ah, bl, dims) + mul(al, bh, dims))


def np_halves(x):
    x = np.asarray(x, np.float32)
    high = x.astype(BF16)
    return np.stack([high, (x - high.astype(np.float32)).astype(BF16)])


def np_turn(count, length):
    position = np.arange(count)
    frequency = np.where(position < count // 2, position, position - count)
    phase = frequency[None, :] * np.arange(length)[:, None] % length
    angle = 2.0 * np.pi / length * phase
    upper = np.stack([np.cos(angle), -np.sin(angle)], axis=1)
    lower = np.stack([np.sin(angle), np.cos(angle)], axis=1)
    return np.stack([upper, lower])


def np_depth(length, count):
    phase = np.arange(length)[:, None] * np.arange(count)[None, :] % length
    angle = 2.0 * np.pi / length * phase
    return np.stack([np.cos(angle), -np.sin(angle)])


def iota(shape, axis):
    return lax.broadcasted_iota(jnp.int32, shape, axis)


def one_hot(rows, cols, row_of, col_of):
    return row_of(iota((rows, cols), 0)) == col_of(iota((rows, cols), 1))


def spread(weights, dims):
    rows, cols = weights.shape if dims == NN else weights.shape[::-1]
    pick = one_hot(rows * SUB, rows, lambda r: r // SUB, lambda c: c).astype(F32).astype(BF16)
    lay = one_hot(cols * SUB, cols, lambda r: r // SUB, lambda c: c).astype(F32).astype(BF16)
    same = one_hot(rows * SUB, cols * SUB, lambda r: r % SUB, lambda c: c % SUB)
    result = []
    for part in halves(weights):
        tall = mul(pick, part, dims).astype(BF16)
        wide = mul(tall, lay, NT)
        result.append(jnp.where(same, wide, 0.0).astype(BF16))
    return result


def unfold(row, count, width):
    tall = jnp.broadcast_to(row, (count, row.shape[1]))
    return pltpu.roll(tall, 0, 1, stride=width, stride_axis=0)


class Place:
    def __init__(self, px, py):
        self.px, self.py = px, py
        self.p = lax.axis_index("px")
        self.q = lax.axis_index("py")
        self.core = lax.rem(self.q, 2)
        self.side = self.q // 2
        self.mate = {"py": self.q + 1 - 2 * self.core}
        self.cross = {"py": lax.rem(self.q + 2, py)}

    def row_peer(self, step):
        return lax.rem(self.p + step, self.px)

    def col_peer(self, step):
        return lax.rem(self.q + step, self.py)

    def greet(self):
        barrier = pltpu.get_barrier_semaphore()
        for step in range(1, self.px):
            pl.semaphore_signal(barrier, inc=1, device_id={"px": self.row_peer(step)}, device_id_type=MESH)
        for step in range(1, self.py):
            pl.semaphore_signal(barrier, inc=1, device_id={"py": self.col_peer(step)}, device_id_type=MESH)

    def meet(self):
        pl.semaphore_wait(pltpu.get_barrier_semaphore(), self.px + self.py - 2)


def remote(src, dst, send, recv, device):
    return pltpu.make_async_remote_copy(
        src_ref=src, dst_ref=dst, send_sem=send, recv_sem=recv, device_id=device, device_id_type=MESH,
    )


def remote_kernel(px, py, second_ref, flow_ref, cot_ref, tyf_ref, tyb_ref, core_ref, win_ref, wout_ref,
                  first_ref, third_ref, scale_ref, tzf_ref, txf_ref, tzb_ref, txb_ref,
                  out_ref, core_out, pack_out,
                  tile, kron, lines_h, lines_l, modes_h, modes_l, tyf, tyb, core, summed, from_mate, to_cross,
                  from_cross, to_row, gathered, lifted, backed, mixed, core_rows, kernel_rows, grads, back_row,
                  blocks, krono, real_h, real_l, totals, partial, ranks_in, ranks_sum, ranks_col,
                  core_all, pack_sum, pack_row, pack_col,
                  load_sem, table_sem, mate_send, mate_recv, cross_send, cross_recv, row_send, row_recv,
                  brow_send, brow_recv, bcross_send, bcross_recv, bmate_send, bmate_recv, out_sem,
                  rs_send, rs_recv, cs_send, cs_recv, ag_send, ag_recv, bg_send, bg_recv,
                  pr_send, pr_recv, pc_send, pc_recv):
    here = Place(px, py)
    p, q = here.p, here.q
    k = q * px + p
    steps, channels, group, cols, depth = tile.shape
    tiles = steps // 2
    ranks = win_ref.shape[0]
    packs = ranks // 4
    r1, m1 = first_ref.shape
    r3, m3 = third_ref.shape
    r2 = second_ref.shape[0]
    wide = packs * LANES

    here.greet()

    def load(t):
        source = flow_ref if t < tiles else cot_ref
        pltpu.make_async_copy(
            source.at[:, pl.ds((t % tiles) * group, group)], tile.at[t], load_sem.at[t]).start()

    load(0)
    tables = [pltpu.make_async_copy(tyf_ref.at[q], tyf, table_sem.at[0]),
              pltpu.make_async_copy(tyb_ref.at[q], tyb, table_sem.at[1]),
              pltpu.make_async_copy(core_ref, core, table_sem.at[2])]
    tables[0].start()
    load(1)
    for f, weight in enumerate((win_ref, wout_ref)):
        high, low = spread(weight[...], NN)
        kron[f, :ranks * SUB] = high
        kron[f, ranks * SUB:] = low
    totals[...] = jnp.zeros_like(totals)
    for t in range(2, steps):
        load(t)
    tables[1].start()
    tables[0].wait()

    def mate_copies(t):
        return [remote(summed.at[t, 2 * s + 1 - here.core], from_mate.at[t, s],
                       mate_send.at[t, s], mate_recv.at[t, s], here.mate) for s in range(2)]

    def cross_copy(t):
        return remote(to_cross.at[t], from_cross.at[t], cross_send.at[t], cross_recv.at[t], here.cross)

    def row_copy(t, step):
        return remote(to_row.at[t, here.row_peer(step)], gathered.at[t // tiles, p, lax.rem(t, tiles)],
                      row_send.at[t, step], row_recv.at[t, step], {"px": here.row_peer(step)})

    def compute(t):
        f = t // tiles

        def lift(x, carry):
            sides = [tile[t, :, x, h * SUB:(h + 1) * SUB, :].reshape(channels * SUB, depth)
                     for h in range(cols // SUB)]
            both = mul(kron[f], jnp.concatenate(sides, axis=1))
            high, low = halves(both[:ranks * SUB] + both[ranks * SUB:])
            for a in range(ranks):
                for h in range(cols // SUB):
                    row = pl.multiple_of(x * (packs * cols) + (a // 4) * cols + h * SUB, SUB)
                    spot = (pl.ds(row, SUB), slice((a % 4) * depth, (a % 4 + 1) * depth))
                    part = (slice(a * SUB, (a + 1) * SUB), slice(h * depth, (h + 1) * depth))
                    lines_h[spot] = high[part]
                    lines_l[spot] = low[part]
            return carry

        lax.fori_loop(0, group, lift, 0)
        modes = mul3((lines_h[...], lines_l[...]), (tzf_ref[0], tzf_ref[1]))
        high, low = halves(modes)
        for x in range(group):
            for a in range(packs):
                for o in range(2):
                    spot = (slice((x * 2 + o) * cols, (x * 2 + o + 1) * cols), slice(a * LANES, (a + 1) * LANES))
                    part = (slice((x * packs + a) * cols, (x * packs + a + 1) * cols),
                            slice(o * LANES, (o + 1) * LANES))
                    modes_h[spot] = high[part]
                    modes_l[spot] = low[part]
        total = mul3((tyf[0], tyf[1]), (modes_h[...], modes_l[...]))
        summed[t] = total.reshape(summed.shape[1:])

    def kernel_side():
        tables[2].wait()

        def one(a, carry):
            for r in range(r1):
                total = second_ref[0, k] * core[a, r, 0]
                for s in range(1, r2):
                    total = total + second_ref[s, k] * core[a, r, s]
                core_rows[pl.ds(pl.multiple_of((a * r1 + r) * r3, r3), r3), :ranks] = total
            return carry

        core_rows[...] = jnp.zeros_like(core_rows)
        lax.fori_loop(0, ranks, one, 0)
        kernel_rows[...] = exact(folded(), widen())

    def folded():
        total = core_rows[pl.ds(0, ranks * r1, stride=r3), :]
        for t in range(1, r3):
            total = total + pltpu.roll(core_rows[pl.ds(t, ranks * r1, stride=r3), :], (r3 - t) * ranks, 1)
        return total

    def widen():
        tall = one_hot(LANES, r3, lambda r: (r3 - r // ranks) % r3, lambda c: c).astype(F32)
        flat = one_hot(m3, wide, lambda r: r, lambda c: c % m3).astype(F32)
        full = exact(exact(tall, third_ref[...]), flat)
        return jnp.where(one_hot(LANES, wide, lambda r: r % ranks, lambda c: c // m3), full, 0.0)

    def body(t, carry):
        @pl.when(t < steps)
        def _():
            pltpu.make_async_copy(flow_ref.at[:, pl.ds(0, group)], tile.at[t], load_sem.at[t]).wait()
            compute(t)

        @pl.when(t == 0)
        def _():
            here.meet()
            tables[2].start()

        @pl.when(t < steps)
        def _():
            for copy in mate_copies(t):
                copy.start()

        @pl.when((t >= 1) & (t < steps + 1))
        def _():
            u = t - 1
            for copy in mate_copies(u):
                copy.wait_recv()
            to_cross[u] = summed[u, 2 * (1 - here.side) + here.core] + from_mate[u, 1 - here.side]
            cross_copy(u).start()

        @pl.when(t == steps)
        def _():
            kernel_side()

        @pl.when(t >= 3)
        def _():
            u = t - 3
            cross_copy(u).wait_recv()
            to_row[u] = summed[u, 2 * here.side + here.core] + from_mate[u, here.side] + from_cross[u]
            for step in range(1, px):
                row_copy(u, step).start()
            gathered[u // tiles, p, lax.rem(u, tiles)] = to_row[u, p]

        return carry

    lax.fori_loop(0, steps + 3, body, 0)
    scale = scale_ref[...]

    def arrive(f):
        for t in range(f * tiles, (f + 1) * tiles):
            for step in range(1, px):
                row_copy(t, step).wait_recv()
        lines = mul3((txf_ref[0], txf_ref[1]), halves(gathered[f].reshape(-1, wide)))
        for o in range(2):
            for a in range(packs):
                cell = lines[o * m1:(o + 1) * m1, a * LANES:(a + 1) * LANES]
                if f == 0:
                    lifted[o, a] = cell
                else:
                    backed[o, a] = cell * scale

    group_of = iota((m1, LANES), 1) // m3
    lay = one_hot(r1 * LANES, r1, lambda r: r // LANES, lambda c: c).astype(F32)
    columns = exact(first_ref[...], lay, (((0,), (1,)), ((), ())))
    mixed[...] = jnp.zeros_like(mixed)

    def around(v):
        v = v + pltpu.roll(v, 64, 1)
        return v + pltpu.roll(v, 32, 1)

    def spots(a):
        return [pl.ds(pl.multiple_of((a * packs + b) * LANES, LANES), LANES) for b in range(packs)]

    def blend(a, carry):
        mine = group_of == lax.rem(a, 4)
        block = kernel_rows[pl.ds(pl.multiple_of(a * r1, r1), r1), :]
        lift = [around(jnp.where(mine, lifted[o, a // 4], 0.0)) for o in range(2)]
        for b, lanes in enumerate(spots(a)):
            total = columns[:, :LANES] * block[0:1, b * LANES:(b + 1) * LANES]
            for r in range(1, r1):
                total = total + columns[:, r * LANES:(r + 1) * LANES] * block[r:r + 1, b * LANES:(b + 1) * LANES]
            grads[:, lanes] = total
            for o in range(2):
                mixed[0, o, b] += total * lift[o]
        return carry

    def unblend(a, carry):
        mine = group_of == lax.rem(a, 4)
        lift = [around(jnp.where(mine, lifted[o, a // 4], 0.0)) for o in range(2)]
        sums = [None, None]
        for b, lanes in enumerate(spots(a)):
            total = grads[:, lanes]
            grad = None
            for o in range(2):
                back = backed[o, b]
                term = total * back
                sums[o] = term if sums[o] is None else sums[o] + term
                term = lift[o] * back
                grad = term if grad is None else grad + term
            grads[:, lanes] = grad
        for o in range(2):
            mixed[1, o, a // 4] += jnp.where(mine, around(sums[o]), 0.0)
        return carry

    def brow_copy(t, step):
        to = here.row_peer(step)
        return remote(back_row.at[t // tiles, to, lax.rem(t, tiles)], blocks.at[t, q, p],
                      brow_send.at[t, step], brow_recv.at[t, step], {"px": to})

    def bcross_copy(t):
        return remote(blocks.at[t, q], blocks.at[t, q], bcross_send.at[t], bcross_recv.at[t], here.cross)

    def bmate_copy(t, s):
        quarter = q if s == 0 else lax.rem(q + 2, py)
        return remote(blocks.at[t, quarter], blocks.at[t, quarter],
                      bmate_send.at[t, s], bmate_recv.at[t, s], here.mate)

    share = partial.shape[0] // px

    def rs_copy(step):
        to = here.row_peer(step)
        return remote(partial.at[pl.ds(to * share, share)], ranks_in.at[p], rs_send.at[step], rs_recv.at[step],
                      {"px": to})

    def cs_copy(step):
        to = here.col_peer(step)
        return remote(ranks_sum.at[to], ranks_col.at[q], cs_send.at[step], cs_recv.at[step], {"py": to})

    def ag_copy(step):
        return remote(core_all.at[p, q], core_all.at[p, q], ag_send.at[step], ag_recv.at[step],
                      {"px": here.row_peer(step)})

    def bg_copy(s):
        quarter = lax.rem(q + 2, py) if s == 2 else q
        return remote(core_all.at[:, quarter], core_all.at[:, quarter], bg_send.at[s], bg_recv.at[s],
                      here.cross if s == 0 else here.mate)

    def pr_copy(step):
        return remote(pack_sum.at[0], pack_row.at[p], pr_send.at[step], pr_recv.at[step],
                      {"px": here.row_peer(step)})

    def pc_copy(step):
        return remote(pack_sum.at[1], pack_col.at[q], pc_send.at[step], pc_recv.at[step],
                      {"py": here.col_peer(step)})

    def rows_out(f):
        pieces = [jnp.concatenate([mixed[f, o, b] for b in range(packs)], axis=1) for o in range(2)]
        lines = jnp.concatenate(pieces, axis=0)
        if f == 0:
            lines = lines * jnp.concatenate([scale] * packs, axis=1)
        back_row[f] = mul3((txb_ref[0], txb_ref[1]), halves(lines)).reshape(back_row.shape[1:])
        for t in range(f * tiles, (f + 1) * tiles):
            for step in range(1, px):
                brow_copy(t, step).start()
            blocks[t, q, p] = back_row[f, p, t - f * tiles]

    arrive(0)
    lax.fori_loop(0, ranks, blend, 0)
    rows_out(0)
    arrive(1)
    lax.fori_loop(0, ranks, unblend, 0)
    def tall_grads():
        thin = exact(first_ref[...], grads[...])
        return jnp.concatenate([thin[:, a * wide:(a + 1) * wide] for a in range(ranks)], axis=0)

    def core_side():
        partial[...] = exact(tall_grads(), widen(), NT)
        for step in range(1, px):
            rs_copy(step).start()
        ranks_in[p] = partial[pl.ds(pl.multiple_of(p * share, share), share), :]

    def small_side():
        spread_rows = jnp.concatenate([kernel_rows[a * r1:(a + 1) * r1, :] for a in range(ranks)], axis=1)
        grad_first = exact(spread_rows, grads[...], NT)
        cross = exact(folded(), tall_grads(), TN)
        cross = jnp.where(one_hot(LANES, wide, lambda r: r % ranks, lambda c: c // m3), cross, 0.0)
        cross = cross.reshape(r3, ranks, wide).sum(axis=1)
        cross = exact(one_hot(r3, r3, lambda r: (r3 - r) % r3, lambda c: c).astype(F32), cross)
        grad_third = exact(cross, one_hot(wide, m3, lambda r: r % m3, lambda c: c).astype(F32))
        lane = iota((r1, LANES), 1)
        row = iota((r1, LANES), 0)
        small = exact(grad_first, one_hot(m1, LANES, lambda r: r, lambda c: c).astype(F32))
        small = small + exact(grad_third, one_hot(m3, LANES, lambda r: r + m1, lambda c: c).astype(F32))

        def second(a, sums):
            rows = partial[pl.ds(pl.multiple_of(a * r1, r1), r1), :]
            sums = list(sums)
            for r in range(r1):
                cell = unfold(rows[r:r + 1], r3, ranks)[:, :ranks]
                for s in range(r2):
                    sums[s] = sums[s] + core[a, r, s] * cell
            return tuple(sums)

        sums = lax.fori_loop(0, ranks, second, tuple(jnp.zeros((r3, ranks), F32) for _ in range(r2)))
        for s in range(r2):
            small = small + jnp.where((lane == k + m1 + m3) & (row == s), jnp.sum(sums[s]), 0.0)
        pack_sum[0, ranks:ranks + r1] = small

    core_side()
    rows_out(1)
    tables[1].wait()

    def slot(t):
        return (t + 1) * (1 - t // tiles)

    def place(t):
        here_slot = slot(t)
        high, low = halves(blocks[t].reshape(-1, wide))
        modes = mul3((tyb[0], tyb[1]), (high, low))
        high, low = halves(modes)
        for x in range(group):
            for a in range(packs):
                for o in range(2):
                    part = (slice((x * 2 + o) * cols, (x * 2 + o + 1) * cols), slice(a * LANES, (a + 1) * LANES))
                    spot = (slice((x * packs + a) * cols, (x * packs + a + 1) * cols),
                            slice(o * LANES, (o + 1) * LANES))
                    lines_h[spot] = high[part]
                    lines_l[spot] = low[part]
        half = 2 * LANES
        real = mul3((lines_h[:, :half], lines_l[:, :half]), (tzb_ref[0], tzb_ref[1]))
        high, low = halves(real)
        for x in range(group):
            for a in range(ranks):
                for h in range(cols // SUB):
                    row = (x * packs + a // 4) * cols + h * SUB
                    part = (slice(row, row + SUB), slice((a % 4) * depth, (a % 4 + 1) * depth))
                    spot = (here_slot, x, slice(a * SUB, (a + 1) * SUB), slice(h * depth, (h + 1) * depth))
                    real_h[spot] = high[part]
                    real_l[spot] = low[part]

    def outer(t):
        u = lax.rem(t + tiles, steps)

        def one(x, carry):
            sides = [tile[u, :, x, h * SUB:(h + 1) * SUB, :].reshape(channels * SUB, depth)
                     for h in range(cols // SUB)]
            cells = jnp.concatenate(sides, axis=1)
            totals[u // tiles] += mul(cells, real_h[slot(t), x], NT) + mul(cells, real_l[slot(t), x], NT)
            return carry

        lax.fori_loop(0, group, one, 0)

    def out_copy(g):
        return pltpu.make_async_copy(tile.at[tiles + g], out_ref.at[:, pl.ds(g * group, group)], out_sem.at[g])

    def emit(g, carry):
        def one(x, carry):
            both = mul3((krono[0], krono[1]), (real_h[g + 1, x], real_l[g + 1, x])).astype(BF16)
            for h in range(cols // SUB):
                tile[tiles + g, :, x, h * SUB:(h + 1) * SUB, :] = both[:, h * depth:(h + 1) * depth].reshape(
                    channels, SUB, depth)
            return carry

        lax.fori_loop(0, group, one, 0)
        out_copy(g).start()
        return carry

    def back_body(i, carry):
        @pl.when(i < steps)
        def _():
            for step in range(1, px):
                brow_copy(i, step).wait_recv()
            bcross_copy(i).start()
            bmate_copy(i, 0).start()

        @pl.when((i >= 2) & (i < steps + 2))
        def _():
            bcross_copy(i - 2).wait_recv()
            bmate_copy(i - 2, 1).start()

        @pl.when(i >= 3)
        def _():
            t = i - 3
            for s in range(2):
                bmate_copy(t, s).wait_recv()
            place(t)
            outer(t)

        @pl.when(i == 0)
        def _():
            small_side()

        @pl.when(i == 1)
        def _():
            high, low = spread(wout_ref[...], NT)
            krono[0] = high
            krono[1] = low

        @pl.when(i == 5)
        def _():
            for step in range(1, px):
                rs_copy(step).wait_recv()
            for s in range(r2):
                total = None
                for o in range(px):
                    term = ranks_in[o] * second_ref[s, q * px + o]
                    total = term if total is None else total + term
                ranks_sum[s // 2, s % 2] = total
            ranks_col[q] = ranks_sum[q]
            for step in range(1, py):
                cs_copy(step).start()

        @pl.when(i == 7)
        def _():
            for step in range(1, py):
                cs_copy(step).wait_recv()
            total = ranks_col[0]
            for s in range(1, py):
                total = total + ranks_col[s]
            core_all[p, q] = total
            for step in range(1, px):
                ag_copy(step).start()

        @pl.when(i == 9)
        def _():
            for step in range(1, px):
                ag_copy(step).wait_recv()
            bg_copy(0).start()
            bg_copy(1).start()

        return carry

    lax.fori_loop(0, steps + 3, back_body, 0)
    bg_copy(0).wait_recv()
    bg_copy(2).start()
    keep = one_hot(channels * SUB, ranks * SUB, lambda r: r % SUB, lambda c: c % SUB)
    grids = [jnp.where(keep, totals[f], 0.0).reshape(channels, SUB, ranks * SUB).sum(axis=1) for f in range(2)]
    pick = one_hot(ranks, ranks * SUB, lambda r: r, lambda c: c // SUB).astype(F32)
    pack_sum[0, :ranks] = exact(pick, jnp.concatenate(grids, axis=0), NT)
    for step in range(1, px):
        pr_copy(step).start()
    pack_row[p] = pack_sum[0]
    lax.fori_loop(0, tiles // 2, emit, 0)
    bg_copy(1).wait_recv()
    bg_copy(2).wait_recv()
    core_out[...] = core_all[...]
    for step in range(1, px):
        pr_copy(step).wait_recv()
    total = pack_row[0]
    for s in range(1, px):
        total = total + pack_row[s]
    pack_sum[1] = total
    for step in range(1, py):
        pc_copy(step).start()
    pack_col[q] = total
    lax.fori_loop(tiles // 2, tiles, emit, 0)

    def drain(t, carry):
        for copy in mate_copies(t):
            copy.wait_send()
        cross_copy(t).wait_send()
        bcross_copy(t).wait_send()
        for s in range(2):
            bmate_copy(t, s).wait_send()
        for step in range(1, px):
            row_copy(t, step).wait_send()
            brow_copy(t, step).wait_send()
        return carry

    lax.fori_loop(0, steps, drain, 0)
    for step in range(1, px):
        for copy in (rs_copy, ag_copy, pr_copy):
            copy(step).wait_send()
    for s in range(3):
        bg_copy(s).wait_send()
    for step in range(1, py):
        cs_copy(step).wait_send()
        pc_copy(step).wait_recv()
    total = pack_col[0]
    for s in range(1, py):
        total = total + pack_col[s]
    pack_out[...] = total
    for step in range(1, py):
        pc_copy(step).wait_send()
    for g in range(tiles):
        out_copy(g).wait()


def emit_kernel(field_ref, core_ref, pack_ref, out_ref, core_out, in_out, oo_out,
                first_out, second_out, third_out, tile, core, load_sem, store_sem, core_sem):
    ranks, channels = in_out.shape
    _, r1, r2, r3, _ = core_out.shape
    m1, m3 = first_out.shape[1], third_out.shape[1]
    m2 = second_out.shape[1]
    tiles, _, group = tile.shape[:3]
    per = core_ref.shape[2]
    share = ranks // tiles
    pair = core_ref.shape[3] // r1

    def load(g):
        return pltpu.make_async_copy(field_ref.at[:, pl.ds(g * group, group)], tile.at[g], load_sem.at[g])

    def store(g):
        return pltpu.make_async_copy(tile.at[g], out_ref.at[:, pl.ds(g * group, group)], store_sem.at[g])

    def lay(g):
        part = pl.ds(g * share, share)
        return pltpu.make_async_copy(core.at[part], core_out.at[part], core_sem.at[g])

    for g in range(tiles):
        load(g).start()

    def one(a, carry):
        for s in range(r2):
            spot = pl.ds(pl.multiple_of(lax.rem(a, pair) * r1, r1), r1)
            rows = core_ref[a // pair, s // per, s % per, spot, :]
            for r in range(r1):
                core[a, r, s] = unfold(rows[r:r + 1], r3, ranks)[:, :ranks]
        return carry

    for g in range(tiles):
        lax.fori_loop(g * share, (g + 1) * share, one, 0)
        lay(g).start()
        load(g).wait()
        store(g).start()
    in_out[...] = pack_ref[:ranks, :channels]
    oo_out[...] = pack_ref[:ranks, channels:2 * channels]
    first_out[...] = pack_ref[ranks:ranks + r1, :m1]
    third_out[...] = pack_ref[ranks:ranks + r1, m1:m1 + m3]
    second_out[...] = pack_ref[ranks:ranks + r1, m1 + m3:m1 + m3 + m2]
    for g in range(tiles):
        lay(g).wait()
        store(g).wait()


def fast_shards(px, py, flow_field, cotangent, tucker_core, in_factor, out_factor,
                first_factor, second_factor, third_factor):
    channels, rows, cols, depth = flow_field.shape
    ri, ro, r1, r2, r3 = tucker_core.shape
    group = 2 * LANES // (2 * cols)
    tiles = rows // group
    steps = 2 * tiles
    packs = ri // 4
    wide = packs * LANES
    keep = px
    inverse_count = 1.0 / (NX * NY * NZ)

    small = np_depth(NZ, M3)
    tz = np.einsum("st,pzm->szptm", np.eye(4), small).reshape(4 * depth, 2 * 4 * M3)
    turn = np_turn(M2, NY).reshape(2, py, cols, 2, py, keep)
    ty = np.einsum("pdyoqk,xw->dqkxowpy", turn, np.eye(group))
    ty = ty.reshape(py, py * keep * group * 2, group * 2 * cols)
    turn = np_turn(M1, NX).reshape(2, NX, 2, M1)
    tx = turn.transpose(2, 3, 1, 0).reshape(2 * M1, NX * 2)
    tz_f, tz_b = np_halves(tz), np_halves(tz.T)
    ty_f = np_halves(ty).swapaxes(0, 1)
    ty_b = np_halves(ty.swapaxes(1, 2)).swapaxes(0, 1)
    tx_f, tx_b = np_halves(tx), np_halves(tx.T)
    weight = np.where(np.arange(M3) == 0, 1.0, 2.0) * inverse_count
    scale = jnp.asarray(np.tile(weight, 4)[None, :].astype(np.float32))

    vmem = pl.BlockSpec(memory_space=pltpu.VMEM)
    smem = pl.BlockSpec(memory_space=pltpu.SMEM)
    anywhere = pl.BlockSpec(memory_space=pl.ANY)
    shape = jax.ShapeDtypeStruct
    dma = pltpu.SemaphoreType.DMA

    def buf(*dims):
        return pltpu.VMEM(dims, F32)

    def thin(*dims):
        return pltpu.VMEM(dims, BF16)

    lines = group * packs * cols
    block = (keep, 2 * group, wide)
    real = (group, ri * SUB, cols // SUB * depth)
    count = ri * r1
    spectrum = (2, packs, M1, LANES)
    piece = (r2 // py, count // px, LANES)
    pack = (ri + r1, LANES)
    core = tucker_core.transpose(0, 2, 3, 4, 1)
    field, core_sum, packed = pl.pallas_call(
        functools.partial(remote_kernel, px, py),
        out_shape=(shape(flow_field.shape, BF16), shape((px, py) + piece, F32), shape(pack, F32)),
        in_specs=[smem] + [anywhere] * 5 + [vmem] * 9,
        out_specs=(anywhere, vmem, vmem),
        scratch_shapes=[
            thin(steps, channels, group, cols, depth),
            thin(2, 2 * ri * SUB, channels * SUB),
            thin(lines, 4 * depth), thin(lines, 4 * depth),
            thin(group * 2 * cols, wide), thin(group * 2 * cols, wide),
            thin(*ty_f.shape[1:]), thin(*ty_b.shape[1:]), buf(*core.shape),
            buf(steps, py, *block), buf(steps, 2, *block), buf(steps, *block), buf(steps, *block),
            buf(steps, *block), buf(2, px, tiles, 2 * group, wide),
            buf(*spectrum), buf(*spectrum), buf(2, *spectrum),
            buf(count * r3, LANES), buf(count, wide), buf(M1, ri * wide),
            buf(2, px, tiles, 2 * group, wide), buf(steps, py, *block),
            thin(2, channels * SUB, ro * SUB), thin(tiles + 1, *real), thin(tiles + 1, *real),
            buf(2, channels * SUB, ri * SUB),
            buf(count, LANES), buf(px, count // px, LANES), buf(py, *piece), buf(py, *piece),
            buf(px, py, *piece), buf(2, *pack), buf(px, *pack), buf(py, *pack),
            dma((steps,)), dma((3,)),
            dma((steps, 2)), dma((steps, 2)), dma((steps,)), dma((steps,)), dma((steps, px)), dma((steps, px)),
            dma((steps, px)), dma((steps, px)), dma((steps,)), dma((steps,)), dma((steps, 2)), dma((steps, 2)),
            dma((tiles,)),
            dma((px,)), dma((px,)), dma((py,)), dma((py,)), dma((px,)), dma((px,)), dma((3,)), dma((3,)),
            dma((px,)), dma((px,)), dma((py,)), dma((py,)),
        ],
        compiler_params=pltpu.CompilerParams(
            vmem_limit_bytes=VMEM_LIMIT, collective_id=0, has_side_effects=True),
    )(second_factor.T, flow_field, cotangent, jnp.asarray(ty_f), jnp.asarray(ty_b), core, in_factor.T,
      out_factor.T, first_factor.T, third_factor.T, scale,
      jnp.asarray(tz_f), jnp.asarray(tx_f), jnp.asarray(tz_b), jnp.asarray(tx_b))

    out, core_grad, in_grad, out_grad, first_grad, second_grad, third_grad = pl.pallas_call(
        emit_kernel,
        out_shape=(
            shape(flow_field.shape, BF16), shape(core.shape, F32), shape((ri, channels), F32),
            shape((ro, channels), F32), shape((r1, M1), F32), shape((r2, M2), F32), shape((r3, M3), F32),
        ),
        in_specs=[anywhere, vmem, vmem],
        out_specs=(anywhere, anywhere) + (vmem,) * 5,
        scratch_shapes=[
            thin(tiles, channels, group, cols, depth), buf(*core.shape),
            dma((tiles,)), dma((tiles,)), dma((tiles,)),
        ],
        compiler_params=pltpu.CompilerParams(vmem_limit_bytes=VMEM_LIMIT),
    )(field, core_sum, packed)
    return (out, core_grad.transpose(0, 4, 1, 2, 3), in_grad.T, out_grad.T, first_grad.T, second_grad.T,
            third_grad.T)


def solution(mesh):
    px, py = mesh.shape["px"], mesh.shape["py"]
    rows, cols = NX // px, NY // py
    fits = py == 4 and px * py == M2 and cols == 32 and rows == 16 and NZ == LANES
    fits = fits and M1 == 32 and M3 == 32
    body = functools.partial(fast_shards, px, py) if fits else shards
    return jax.shard_map(
        body,
        mesh=mesh,
        in_specs=(
            P(None, "px", "py", None),
            P(None, "px", "py", None),
            P(),
            P(),
            P(),
            P(),
            P(),
            P(),
        ),
        out_specs=(P(None, "px", "py", None), P(), P(), P(), P(), P(), P()),
        check_vma=False,
    )
```
